128 devices in a mesh: gx: 4 (over y_lo, core), gy: 8 (over x, y_hi), gz: 4 (over z).
Axes of the slice: x: 4, y: 4 (y_hi: 2, y_lo: 2; y = y_hi * 2 + y_lo), z: 4, core: 2. Of those that a mesh axis runs over, the one named last changes fastest.
Arguments:
- positions: float32 [3, 4, 8, 4, 4096], P(None, 'gx', 'gy', 'gz'), may hold values from 0 to 4, as said below
- velocities: float32 [3, 4, 8, 4, 4096], P(None, 'gx', 'gy', 'gz'), may hold values from -6 to 6
- strength: float32 [4, 8, 4, 4096], P('gx', 'gy', 'gz'), may hold values from 0.5 to 2
- charge: float32 [4, 8, 4, 4096], P('gx', 'gy', 'gz'), may hold values from -5 to 5
- bond_stiffness: float32 [2, 4, 8, 4, 4096], P(None, 'gx', 'gy', 'gz'), may hold values from 0.5 to 4
- bond_partner: int32 [2, 4, 8, 4, 4096], P(None, 'gx', 'gy', 'gz'), may hold values from 0 to 18431, as said below
- pair_blocks: int32 [4, 8, 4, 32, 8], P('gx', 'gy', 'gz'), may hold values from 0 to 143, as said below
- tile_count: int32 [4, 8, 4], P('gx', 'gy', 'gz'), may hold values from 1024 to 4096, as said below
- block_cell: int32 [4, 8, 4, 32], P('gx', 'gy', 'gz'), may hold values from 0 to 1023
- cell_frac: float32 [3, 1024], replicated, may hold values from 0 to 1
- bond_force: float32 [3, 4, 8, 4, 4096], P(None, 'gx', 'gy', 'gz'), may hold values from -6 to 6
- pair_force: float32 [3, 4, 8, 4, 4096], P(None, 'gx', 'gy', 'gz'), may hold values from -6 to 6
- far_force: float32 [3, 4, 8, 4, 4096], P(None, 'gx', 'gy', 'gz'), may hold values from -6 to 6
Outputs:
- positions_out: float32 [3, 4, 8, 4, 4096], P(None, 'gx', 'gy', 'gz')
- velocities_out: float32 [3, 4, 8, 4, 4096], P(None, 'gx', 'gy', 'gz')
The draws below stay inside these ranges and needn't reach their ends.
Inputs may be any that keep to these rules, and one draw needn't show every extreme that they name: `positions`: each bead lies inside the unit cube of its block. `tile_count`: live beads of a tile fill its slots from 0 upward; some tile is full in every draw. `bond_partner`: A live bead's partners are live beads of its own block or of one of the six blocks sharing a face with it; an empty slot names its own column. `pair_blocks`: each row begins with the block itself and then lists distinct blocks that share a face, an edge or a corner with it.
All inputs are finite; a program needn't handle non-finite values.
Results may differ from the reference program's by a relative error of at most 0.0003.
Values sent between devices are 32-bit elements; how exact they have to be, the bound alone decides.
A program may use at most 64 MiB of HBM per device.

```python
import math
import jax
import jax.numpy as jnp
from jax import lax

SBX = 4
SBY = 4
SBZ = 2
BLK = 128
KN = 8
NB = 32
BT = 4096
NTX = 4
NTY = 8
NTZ = 4
CELLS = 1024


def block_places():
    block_ids = jnp.arange(SBX * SBY * SBZ, dtype=jnp.int32)
    return (block_ids // (SBY * SBZ), block_ids // SBZ % SBY, block_ids % SBZ)


def extended_block(place_x, place_y, place_z):
    return ((place_x + 1) * (SBY + 2) + place_y + 1) * (SBZ + 2) + place_z + 1


def tile_counts(key):
    base_key = jax.random.fold_in(key, 7001)
    counts = jax.random.randint(base_key, (NTX, NTY, NTZ), BT // 4, BT + 1)
    full_pick = jax.random.randint(jax.random.fold_in(base_key, 1), (3,), 0, 1 << 20)
    counts = counts.at[full_pick[0] % NTX, full_pick[1] % NTY, full_pick[2] % NTZ].set(BT)
    return counts.astype(jnp.int32)


def draw_tile_count(key, part):
    return tile_counts(key)


def draw_positions(key, part):
    inside = jax.random.uniform(jax.random.fold_in(key, 7004), (3, NTX, NTY, NTZ, BT), jnp.float32)
    place_x, place_y, place_z = block_places()
    places = jnp.stack([place_x, place_y, place_z], 0).astype(jnp.float32)
    slot_places = jnp.repeat(places, BLK, axis=1)
    return (inside + slot_places[:, None, None, None, :]).astype(jnp.float32)


def draw_bond_partner(key, part):
    counts = tile_counts(key)
    base_key = jax.random.fold_in(key, 7002)
    block_count = SBX * SBY * SBZ
    full_shape = (2, NTX, NTY, NTZ, block_count, BLK)
    choose_bits = jax.random.randint(jax.random.fold_in(base_key, 1), full_shape, 0, 24)
    face_pick = jnp.where(choose_bits < 18, 0, choose_bits - 17)
    face_moves = ((0, 0, 0), (-1, 0, 0), (1, 0, 0), (0, -1, 0), (0, 1, 0), (0, 0, -1), (0, 0, 1))
    place_x, place_y, place_z = block_places()
    tile_x = jnp.arange(NTX, dtype=jnp.int32)[:, None, None, None]
    tile_y = jnp.arange(NTY, dtype=jnp.int32)[None, :, None, None]
    tile_z = jnp.arange(NTZ, dtype=jnp.int32)[None, None, :, None]
    own_live = jnp.clip(counts[:, :, :, None] - jnp.arange(block_count, dtype=jnp.int32)[None, None, None, :] * BLK, 0, BLK)
    own_ext = extended_block(place_x, place_y, place_z)
    slot_limit = jnp.ones(full_shape, jnp.int32)
    where_block = jnp.zeros(full_shape, jnp.int32)
    for face_index in range(7):
        step_x, step_y, step_z = face_moves[face_index]
        moved_x = place_x + step_x
        moved_y = place_y + step_y
        moved_z = place_z + step_z
        source_x = (tile_x + moved_x[None, None, None, :] // SBX) % NTX
        source_y = (tile_y + moved_y[None, None, None, :] // SBY) % NTY
        source_z = (tile_z + moved_z[None, None, None, :] // SBZ) % NTZ
        source_block = (moved_x % SBX * SBY + moved_y % SBY) * SBZ + moved_z % SBZ
        source_count = counts[source_x, source_y, source_z]
        live_there = jnp.clip(source_count - source_block[None, None, None, :] * BLK, 0, BLK)
        ext_there = extended_block(moved_x, moved_y, moved_z)
        usable = live_there > 0
        limit_here = jnp.where(usable, live_there, own_live)
        ext_here = jnp.where(usable, ext_there[None, None, None, :], own_ext[None, None, None, :])
        chosen = face_pick == face_index
        slot_limit = jnp.where(chosen, limit_here[None, :, :, :, :, None], slot_limit)
        where_block = jnp.where(chosen, ext_here[None, :, :, :, :, None], where_block)
    raw_bits = jax.random.randint(jax.random.fold_in(base_key, 2), full_shape, 0, 1 << 30)
    slot_pick = raw_bits % jnp.maximum(slot_limit, 1)
    partner = (where_block * BLK + slot_pick).reshape(2, NTX, NTY, NTZ, BT)
    slot_ids = jnp.arange(BT, dtype=jnp.int32)
    live_slot = slot_ids[None, None, None, None, :] < counts[None, :, :, :, None]
    itself = jnp.repeat(own_ext, BLK) * BLK + slot_ids % BLK
    return jnp.where(live_slot, partner, itself[None, None, None, None, :]).astype(jnp.int32)


def draw_pair_blocks(key, part):
    block_count = SBX * SBY * SBZ
    base_key = jax.random.fold_in(key, 7003)
    moves = []
    for step_x in (-1, 0, 1):
        for step_y in (-1, 0, 1):
            for step_z in (-1, 0, 1):
                if step_x != 0 or step_y != 0 or step_z != 0:
                    moves.append((step_x, step_y, step_z))
    place_x, place_y, place_z = block_places()
    table = jnp.stack([extended_block(place_x + m[0], place_y + m[1], place_z + m[2]) for m in moves], 1)
    scores = jax.random.randint(base_key, (NTX, NTY, NTZ, block_count, 26), 0, 1 << 30)
    order_ids = jnp.argsort(scores, axis=-1, stable=True)[..., :KN - 1]
    picked = jnp.take_along_axis(jnp.broadcast_to(table, (NTX, NTY, NTZ, block_count, 26)), order_ids, axis=-1)
    own_ext = jnp.broadcast_to(extended_block(place_x, place_y, place_z)[:, None], (NTX, NTY, NTZ, block_count, 1))
    return jnp.concatenate([own_ext, picked], -1).astype(jnp.int32)


def with_ends(values, rng, smallest, high):
    dims = values.shape
    place = [jax.random.randint(jax.random.fold_in(rng, axis), (), 0, dims[axis]) for axis in range(len(dims))]
    values = values.at[tuple(place)].set(smallest)
    longest = dims.index(max(dims))
    place[longest] = (place[longest] + 1) % dims[longest]
    return values.at[tuple(place)].set(high)


def block_levels(rng, dims, cuts, least, largest):
    level, own = 1.0, jax.random.fold_in(rng, 6)
    for position, blocks in cuts:
        steps = jnp.exp(jax.random.uniform(jax.random.fold_in(own, position), (blocks,), jnp.float32, least / len(cuts), largest / len(cuts)))
        level = level * jnp.repeat(steps, dims[position] // blocks).reshape([-1 if axis == position else 1 for axis in range(len(dims))])
    return level


def normal_values(own_key, shape, deviation, most, split=(), kind=jnp.bfloat16):
    loudness = block_levels(own_key, shape, split, -0.22, 0.18) if split else 1.0
    values = jax.random.normal(own_key, shape, jnp.float32) * deviation * loudness
    return jnp.minimum(jnp.maximum(values, -most), most).astype(kind)


def setup_inputs(seed: int = 0) -> dict:
    splits = jax.random.split(jax.random.key(seed), 14)
    return {
        "positions": draw_positions(jax.random.fold_in(splits[13], 71), 0),
        "velocities": normal_values(splits[1], (3, NTX, NTY, NTZ, BT), 1.0, 6.0, ((1, 4), (2, 8), (3, 4)), jnp.float32),
        "strength": jnp.clip(jnp.exp(math.log(2.0) - 1.3862944 * jax.random.uniform(splits[2], (NTX, NTY, NTZ, BT), jnp.float32) ** block_levels(splits[2], (NTX, NTY, NTZ, BT), ((0, 4), (1, 8), (2, 4)), -0.2, 0.2)), 0.5, 2.0),
        "charge": normal_values(splits[3], (NTX, NTY, NTZ, BT), 1.0, 5.0, ((0, 4), (1, 8), (2, 4)), jnp.float32),
        "bond_stiffness": jnp.clip(jnp.exp(math.log(4.0) - 2.0794415 * jax.random.uniform(splits[4], (2, NTX, NTY, NTZ, BT), jnp.float32) ** block_levels(splits[4], (2, NTX, NTY, NTZ, BT), ((1, 4), (2, 8), (3, 4)), -0.2, 0.2)), 0.5, 4.0),
        "bond_partner": draw_bond_partner(jax.random.fold_in(splits[13], 71), 0),
        "pair_blocks": draw_pair_blocks(jax.random.fold_in(splits[13], 71), 0),
        "tile_count": draw_tile_count(jax.random.fold_in(splits[13], 71), 0),
        "block_cell": with_ends(jax.random.randint(splits[8], (NTX, NTY, NTZ, NB), 0, CELLS), jax.random.fold_in(splits[8], 1), 0, CELLS - 1).astype(jnp.int32),
        "cell_frac": jnp.clip(jax.random.uniform(splits[9], (3, CELLS), jnp.float32, 0.0, 1.0), 0.0, 1.0),
        "bond_force": normal_values(splits[10], (3, NTX, NTY, NTZ, BT), 1.0, 6.0, ((1, 4), (2, 8), (3, 4)), jnp.float32),
        "pair_force": normal_values(splits[11], (3, NTX, NTY, NTZ, BT), 1.0, 6.0, ((1, 4), (2, 8), (3, 4)), jnp.float32),
        "far_force": normal_values(splits[12], (3, NTX, NTY, NTZ, BT), 1.0, 6.0, ((1, 4), (2, 8), (3, 4)), jnp.float32),
    }


inner_step = 0.1
gauss_width = 0.25
cutoff_radius = 1.0
pair_scale = 0.1
soften = 1.0
coulomb = 0.02
pair_group = 2

def block_force(own_block, others):
    near_pos = own_block[:3]
    far_pos = others[:3]
    cross_term = jnp.dot(near_pos.T, far_pos, precision=lax.Precision.HIGHEST)
    distance = lax.optimization_barrier(jnp.sum(near_pos * near_pos, 0))[:, None] + lax.optimization_barrier(jnp.sum(far_pos * far_pos, 0))[None, :] - 2.0 * cross_term
    taper_term = jnp.where(distance < cutoff_radius * cutoff_radius, jnp.square(1.0 - distance / (cutoff_radius * cutoff_radius)), 0.0)
    weight = jnp.exp(-distance / (2.0 * gauss_width * gauss_width)) * taper_term * others[3][None, :]
    pulled = jnp.dot(weight, far_pos.T, precision=lax.Precision.HIGHEST)
    weight_sum = lax.optimization_barrier(jnp.sum(weight, 1))
    return pair_scale / (gauss_width * gauss_width) * own_block[3][None, :] * (near_pos * weight_sum[None, :] - pulled.T)

def pair_tile(neighbourhood, blocks, own_packed):
    block_count = blocks.shape[0]
    rows_count = neighbourhood.shape[0]
    grouped = neighbourhood.reshape(rows_count, -1, BLK)
    own_rows = own_packed.reshape(rows_count, block_count, BLK)
    mine_all = jnp.transpose(own_rows, (1, 0, 2)).reshape(block_count // pair_group, pair_group, rows_count, BLK)
    block_lists = blocks.reshape(block_count // pair_group, pair_group, -1)

    def one_block(own_block, chosen):
        others = grouped[:, chosen, :].reshape(rows_count, -1)
        return block_force(own_block, others)

    def one_group(pieces):
        return jax.vmap(one_block)(pieces[0], pieces[1])
    forces = lax.map(one_group, (mine_all, block_lists))
    return jnp.transpose(forces.reshape(block_count, 3, BLK), (1, 0, 2)).reshape(3, -1)

def bond_tile(neighbourhood, partners, stiffness, own_pos):
    result = jnp.zeros_like(own_pos)
    for bond_slot in range(2):
        other_pos = jnp.take(neighbourhood[:3], partners[bond_slot], axis=1)
        result = result - stiffness[bond_slot][None, :] * (own_pos - other_pos)
    return result

def cell_field(totals, centres, targets):
    charge_sum = totals[0]
    dipole = totals[1:4] - charge_sum[None, :] * centres
    separation = targets[:, :, None] - centres[:, None, :]
    inverse = lax.rsqrt(lax.optimization_barrier(jnp.sum(separation * separation, 0)) + soften * soften)
    inverse_cube = inverse * inverse * inverse
    inverse_fifth = inverse_cube * inverse * inverse
    dipole_dot = lax.optimization_barrier(jnp.sum(dipole[:, None, :] * separation, 0))
    field_terms = charge_sum[None, None, :] * separation * inverse_cube - dipole[:, None, :] * inverse_cube + 3.0 * dipole_dot[None] * separation * inverse_fifth
    return lax.optimization_barrier(jnp.sum(field_terms, 2))

def extended_axis(tile_span, sub):
    tiles = jnp.arange(tile_span, dtype=jnp.int32)[:, None]
    cells = jnp.arange(sub + 2, dtype=jnp.int32)[None, :]
    raw = tiles * sub - 1 + cells
    index = (raw % (tile_span * sub)).astype(jnp.int32)
    shift = ((raw // sub - tiles) * sub).astype(jnp.float32)
    return (index, shift)

def neighbourhoods(packed):
    rows_count, size_x, size_y, size_z, bead_count = packed.shape
    grid = packed.reshape(rows_count, size_x, size_y, size_z, SBX, SBY, SBZ, BLK)
    grid = jnp.transpose(grid, (0, 1, 4, 2, 5, 3, 6, 7)).reshape(rows_count, size_x * SBX, size_y * SBY, size_z * SBZ, BLK)
    index_x, shift_x = extended_axis(size_x, SBX)
    index_y, shift_y = extended_axis(size_y, SBY)
    index_z, shift_z = extended_axis(size_z, SBZ)
    grid = jnp.take(grid, index_x.reshape(-1), axis=1)
    grid = jnp.take(grid, index_y.reshape(-1), axis=2)
    grid = jnp.take(grid, index_z.reshape(-1), axis=3)
    grid = grid.reshape(rows_count, size_x, SBX + 2, size_y, SBY + 2, size_z, SBZ + 2, BLK)
    cube_shape = (size_x, SBX + 2, size_y, SBY + 2, size_z, SBZ + 2)
    shift_rows = jnp.stack([jnp.broadcast_to(shift_x[:, :, None, None, None, None], cube_shape), jnp.broadcast_to(shift_y[None, None, :, :, None, None], cube_shape), jnp.broadcast_to(shift_z[None, None, None, None, :, :], cube_shape)], 0)[..., None]
    moved = jnp.concatenate([grid[:3] + shift_rows, grid[3:]], 0)
    moved = jnp.transpose(moved, (1, 3, 5, 0, 2, 4, 6, 7))
    return moved.reshape(size_x * size_y * size_z, rows_count, -1)

def reference(positions, velocities, strength, charge, bond_stiffness, bond_partner, pair_blocks, tile_count, block_cell, cell_frac, bond_force, pair_force, far_force):
    size_x, size_y, size_z, bead_count = strength.shape
    tile_total = size_x * size_y * size_z
    full_shape = positions.shape
    slot_ids = jnp.arange(bead_count, dtype=jnp.int32)
    live_mask = (slot_ids[None, None, None, :] < tile_count[:, :, :, None]).astype(jnp.float32)
    strength_live = strength * live_mask
    charge_live = charge * live_mask
    partners = jnp.transpose(bond_partner.reshape(2, tile_total, bead_count), (1, 0, 2))
    stiffness = jnp.transpose(bond_stiffness.reshape(2, tile_total, bead_count), (1, 0, 2))
    block_lists = pair_blocks.reshape(tile_total, pair_blocks.shape[3], pair_blocks.shape[4])

    def bonds_at(current):
        packed = jnp.concatenate([current, strength_live[None]], 0)
        local_hoods = neighbourhoods(packed)
        own_tiles = jnp.transpose(packed.reshape(4, tile_total, bead_count), (1, 0, 2))

        def one_tile(pieces):
            return bond_tile(pieces[0], pieces[1], pieces[2], pieces[3][:3])
        forces = lax.map(one_tile, (local_hoods, partners, stiffness, own_tiles))
        return (jnp.transpose(forces, (1, 0, 2)).reshape(full_shape), local_hoods, own_tiles)

    def pairs_at(local_hoods, own_tiles):

        def one_tile(pieces):
            return pair_tile(pieces[0], pieces[1], pieces[2])
        forces = lax.map(one_tile, (local_hoods, block_lists, own_tiles))
        return jnp.transpose(forces, (1, 0, 2)).reshape(full_shape)

    def far_at(current):
        corner_x = jnp.broadcast_to(jnp.arange(size_x, dtype=jnp.float32)[:, None, None, None] * SBX, (size_x, size_y, size_z, 1))
        corner_y = jnp.broadcast_to(jnp.arange(size_y, dtype=jnp.float32)[None, :, None, None] * SBY, (size_x, size_y, size_z, 1))
        corner_z = jnp.broadcast_to(jnp.arange(size_z, dtype=jnp.float32)[None, None, :, None] * SBZ, (size_x, size_y, size_z, 1))
        anchor = jnp.stack([corner_x, corner_y, corner_z], 0)
        placed = current + anchor
        block_count = bead_count // BLK
        charge_blocks = charge_live.reshape(size_x, size_y, size_z, block_count, BLK)
        charge_sums = lax.optimization_barrier(jnp.sum(charge_blocks, 4)).reshape(-1)
        weighted = lax.optimization_barrier(jnp.sum((charge_live[None] * placed).reshape(3, size_x, size_y, size_z, block_count, BLK), 5)).reshape(3, -1)
        moments = jnp.concatenate([charge_sums[None], weighted], 0)
        cell_total = cell_frac.shape[1]
        one_hot = (block_cell.reshape(-1)[:, None] == jnp.arange(cell_total, dtype=jnp.int32)[None, :]).astype(jnp.float32)
        totals = jnp.dot(moments, one_hot, precision=lax.Precision.HIGHEST)
        box_size = jnp.array([size_x * SBX, size_y * SBY, size_z * SBZ], dtype=jnp.float32)
        centres = cell_frac * box_size[:, None]
        fields = cell_field(totals, centres, centres)
        block_fields = jnp.dot(fields, one_hot.T, precision=lax.Precision.HIGHEST).reshape(3, size_x, size_y, size_z, block_count)
        return (coulomb * (charge_blocks[None] * block_fields[..., None])).reshape(full_shape)
    half_step = 0.5 * inner_step
    outer_half = 2.0 * inner_step
    current = positions
    velocity_now = velocities + outer_half * far_force + inner_step * pair_force + half_step * bond_force
    bond_now = jnp.zeros_like(current)
    pair_now = jnp.zeros_like(current)
    for inner_index in range(4):
        if inner_index == 2:
            velocity_now = velocity_now + inner_step * pair_now
        if inner_index > 0:
            velocity_now = velocity_now + half_step * bond_now
        current = current + inner_step * velocity_now
        bond_now, local_hoods, own_tiles = bonds_at(current)
        velocity_now = velocity_now + half_step * bond_now
        if inner_index % 2 == 1:
            pair_now = pairs_at(local_hoods, own_tiles)
            velocity_now = velocity_now + inner_step * pair_now
    velocity_now = velocity_now + outer_half * far_at(current)
    return (current, velocity_now)
```

```python
import math

import jax
import jax.numpy as jnp
from jax import lax
from jax.experimental import pallas as pl
from jax.experimental.pallas import tpu as pltpu
from jax.sharding import PartitionSpec as P

MESH = pl.DeviceIdType.MESH
SBX, SBY, SBZ = 4, 4, 2
BLK = 128
NB = SBX * SBY * SBZ
EX, EY, EZ = SBX + 2, SBY + 2, SBZ + 2
NE = EX * EY * EZ
CELLS = 1024
AXES = ("gx", "gy", "gz")

inner_step = 0.1
gauss_width = 0.25
pair_scale = 0.1
soften = 1.0
coulomb = 0.02
half_step = 0.5 * inner_step
outer_half = 2.0 * inner_step

rate = 1.0 / (2.0 * gauss_width * gauss_width)
bits = rate / math.log(2.0)
pair_factor = pair_scale / (gauss_width * gauss_width) * math.exp(-rate) / (bits * bits)

FACES = ((-1, 0, 0), (1, 0, 0), (0, -1, 0), (0, 1, 0), (0, 0, -1), (0, 0, 1))
AROUND = tuple(
    (dx, dy, dz)
    for dx in (-1, 0, 1)
    for dy in (-1, 0, 1)
    for dz in (-1, 0, 1)
    if (dx, dy, dz) != (0, 0, 0)
)
FACE_SLOTS = tuple(AROUND.index(d) for d in FACES)
SIZES = (4, 8, 4)

F32 = jnp.float32
BF16 = jnp.bfloat16


def row_ids(n=4):
    return lax.broadcasted_iota(jnp.int32, (n, BLK), 0)


def rows4(a, b, c, d):
    r = row_ids()
    return jnp.where(r == 0, a, jnp.where(r == 1, b, jnp.where(r == 2, c, d)))


def place(b):
    return b // (SBY * SBZ) + 1, b // SBZ % SBY + 1, b % SBZ + 1


def lane_gather(values, lanes):
    numbers = lax.GatherDimensionNumbers(
        offset_dims=(),
        collapsed_slice_dims=(1,),
        start_index_map=(1,),
        operand_batching_dims=(0,),
        start_indices_batching_dims=(0,),
    )
    return lax.gather(
        values,
        lanes[..., None],
        numbers,
        slice_sizes=(1, 1),
        mode=lax.GatherScatterMode.PROMISE_IN_BOUNDS,
    )


def thirds(value):
    high = value.astype(BF16).astype(F32)
    rest = value - high
    middle = rest.astype(BF16).astype(F32)
    return high, middle, rest - middle


def send_box(step, inner, ghost):
    count = inner
    if step == 0:
        return pl.ds(1, count)
    if ghost:
        return pl.ds(0 if step > 0 else count + 1, 1)
    return pl.ds(count if step > 0 else 1, 1)


def box(direction, ghost):
    return tuple(
        send_box(s, inner, ghost) for s, inner in zip(direction, (SBX, SBY, SBZ))
    )


def kernel(
    pos,
    vel,
    stren,
    chg,
    stiff,
    part,
    bforce,
    pforce,
    fforce,
    frac,
    frac_s,
    pairs,
    cell,
    count,
    xo,
    vo,
    hood0,
    hood1,
    hood2,
    hood3,
    vbuf,
    qbuf,
    near,
    pull,
    left,
    centre,
    part0,
    part1,
    part2,
    got0,
    got1,
    got2,
    hs,
    hr,
    ms,
    mr,
):
    me = tuple(lax.axis_index(a) for a in AXES)

    def device(shift):
        return tuple(lax.rem(m + (s + n), n) for m, s, n in zip(me, shift, SIZES))

    barrier = pltpu.get_barrier_semaphore()
    peers = set(AROUND)
    for axis, n in ((2, 4), (0, 4), (1, 8)):
        for o in range(2, n - 1):
            peers.add(tuple(o if a == axis else 0 for a in range(3)))
    peers = sorted(peers)
    for shift in peers:
        pl.semaphore_signal(barrier, inc=1, device_id=device(shift), device_id_type=MESH)

    rows = row_ids()
    xyz = rows < 3
    lanes = lax.broadcasted_iota(jnp.int32, (1, BLK), 1)

    def halo(hood, which, slots):
        return [
            pltpu.make_async_remote_copy(
                src_ref=hood.at[box(AROUND[d], False)],
                dst_ref=hood.at[box(AROUND[d], True)],
                send_sem=hs.at[which, d],
                recv_sem=hr.at[which, d],
                device_id=device(AROUND[d]),
                device_id_type=MESH,
            )
            for d in slots
        ]

    def arrive(hood, copies, slots):
        for copy, d in zip(copies, slots):
            copy.wait_recv()
            dx, dy, dz = AROUND[d]
            shift = rows4(-SBX * dx * 1.0, -SBY * dy * 1.0, -SBZ * dz * 1.0, 0.0)
            ghost = box(AROUND[d], True)
            hood[ghost] = hood[ghost] + shift

    def begin(b, _):
        px, py, pz = place(b)
        live = jnp.where(b * BLK + lanes < count[0], 1.0, 0.0)
        qbuf[b] = chg[b] * live
        x = rows4(pos[0, b], pos[1, b], pos[2, b], stren[b] * live)
        v = [
            vel[d, b]
            + outer_half * fforce[d, b]
            + inner_step * pforce[d, b]
            + half_step * bforce[d, b]
            for d in range(3)
        ]
        v = rows4(v[0], v[1], v[2], 0.0)
        vbuf[b] = v
        hood0[px, py, pz] = x + inner_step * v
        return 0

    lax.fori_loop(0, NB, begin, 0, unroll=4)
    for d in range(3):
        for k in range(8):
            centre[d, k : k + 1, :] = frac[d : d + 1, k * BLK : (k + 1) * BLK] * (
                1.0 * SIZES[d] * (SBX, SBY, SBZ)[d]
            )

    pl.semaphore_wait(barrier, len(peers))
    copies0 = halo(hood0, 0, FACE_SLOTS)
    for copy in copies0:
        copy.start()

    def bond(hood, b, px, py, pz):
        own = hood[px, py, pz]
        home = (px * EY + py) * EZ + pz
        tiles = [own] + [hood[px + dx, py + dy, pz + dz] for dx, dy, dz in FACES]
        total = jnp.zeros((4, BLK), F32)
        for k in range(2):
            column = part[k, b]
            slot = jnp.broadcast_to(column & (BLK - 1), (4, BLK))
            away = jnp.broadcast_to((column >> 7) - home, (4, BLK))
            other = lane_gather(own, slot)
            for tile, (dx, dy, dz) in zip(tiles[1:], FACES):
                offset = (dx * EY + dy) * EZ + dz
                other = jnp.where(away == offset, lane_gather(tile, slot), other)
            total = total + stiff[k, b] * (other - own)
        return own, jnp.where(xyz, total, 0.0)

    def bond_step(hood, after):
        def body(b, _):
            px, py, pz = place(b)
            own, force = bond(hood, b, px, py, pz)
            v = vbuf[b] + inner_step * force
            vbuf[b] = v
            after[px, py, pz] = own + inner_step * v
            return 0

        lax.fori_loop(0, NB, body, 0, unroll=4)

    def bond_kick(hood, size):
        def body(b, _):
            px, py, pz = place(b)
            _, force = bond(hood, b, px, py, pz)
            vbuf[b] = vbuf[b] + size * force
            return 0

        lax.fori_loop(0, NB, body, 0, unroll=4)

    middle = rows4(0.5 * SBX, 0.5 * SBY, 0.5 * SBZ, 0.0)

    def square_sum(z):
        return jnp.sum(jnp.where(xyz, z * z, 0.0), axis=0, keepdims=True)

    def prepare(hood):
        ones = jnp.where(xyz, 1.0, 0.0)
        blank = jnp.zeros((4, BLK), F32)

        def body(e, _):
            tile = hood[e // (EY * EZ), e // EZ % EY, e % EZ]
            z = tile - middle
            high, mid, low = thirds(jnp.where(xyz, z, -bits * square_sum(z)))
            near[e] = jnp.concatenate(
                [high, mid, low, high, mid, high, ones, blank], axis=0
            ).astype(BF16)
            a = tile[3:4]
            high, mid, low = thirds(jnp.where(xyz, z * a, a))
            pull[e] = jnp.concatenate([high, mid, low, blank], axis=0).astype(BF16)
            return 0

        lax.fori_loop(0, NE, body, 0, unroll=4)

    def prepare_own(hood):
        def body(b, _):
            px, py, pz = place(b)
            z = hood[px, py, pz] - middle
            high, mid, low = thirds(jnp.where(xyz, (2.0 * bits) * z, 1.0))
            ph, pm, pw = thirds(bits - bits * square_sum(z))
            stack = jnp.concatenate(
                [
                    high,
                    high,
                    high,
                    mid,
                    mid,
                    low,
                    rows4(ph, pm, pw, 0.0),
                    jnp.zeros((4, BLK), F32),
                ],
                axis=0,
            )
            left[b] = stack.T.astype(BF16)
            return 0

        lax.fori_loop(0, NB, body, 0, unroll=4)

    def pair(hood, c):
        px, py, pz = place(c)
        mine = left[c]
        acc = jnp.zeros((BLK, 16), F32)
        for k in range(0, 8, 2):
            e0, e1 = pairs[c, k], pairs[c, k + 1]
            t = jnp.dot(
                mine,
                jnp.concatenate([near[e0], near[e1]], axis=1),
                preferred_element_type=F32,
            )
            r = jnp.maximum(t, 0.0)
            w = jnp.exp2(t) * (r * r)
            high = w.astype(BF16)
            low = (w - high.astype(F32)).astype(BF16)
            y = jnp.concatenate([pull[e0], pull[e1]], axis=1)
            over = (((1,), (1,)), ((), ()))
            acc = acc + lax.dot_general(high, y, over, preferred_element_type=F32)
            acc = acc + lax.dot_general(low, y, over, preferred_element_type=F32)
        s = acc.T
        f = s[0:4] + s[4:8] + s[8:12]
        tile = hood[px, py, pz]
        z = tile - middle
        force = (pair_factor * tile[3:4]) * (z * f[3:4] - f)
        return tile, jnp.where(xyz, force, 0.0)

    GROUP = 4

    def pair_step(hood, after):
        def body(g, _):
            for j in range(GROUP):
                c = g * GROUP + j
                px, py, pz = place(c)
                own, force = pair(hood, c)
                v = vbuf[c] + (2.0 * inner_step) * force
                vbuf[c] = v
                after[px, py, pz] = own + inner_step * v
            return 0

        lax.fori_loop(0, NB // GROUP, body, 0)

    def pair_kick(hood, lo, hi):
        def body(g, _):
            for j in range(GROUP):
                c = g * GROUP + j
                _, force = pair(hood, c)
                vbuf[c] = vbuf[c] + inner_step * force
            return 0

        lax.fori_loop(lo // GROUP, hi // GROUP, body, 0)

    arrive(hood0, copies0, FACE_SLOTS)
    bond_step(hood0, hood1)
    every = tuple(range(len(AROUND)))
    copies1 = halo(hood1, 1, every)
    for copy in copies1:
        copy.start()
    prepare_own(hood1)
    arrive(hood1, copies1, every)
    prepare(hood1)
    bond_kick(hood1, inner_step)
    pair_step(hood1, hood2)
    copies2 = halo(hood2, 2, FACE_SLOTS)
    for copy in copies2:
        copy.start()
    arrive(hood2, copies2, FACE_SLOTS)
    bond_step(hood2, hood3)
    copies3 = halo(hood3, 3, every)
    for copy in copies3:
        copy.start()

    cell_ids = lax.broadcasted_iota(jnp.int32, (8, BLK), 0) * BLK + lax.broadcasted_iota(
        jnp.int32, (8, BLK), 1
    )
    corner = rows4(
        (me[0] * SBX).astype(F32), (me[1] * SBY).astype(F32), (me[2] * SBZ).astype(F32), 0.0
    )

    def gather_moments(b, totals):
        px, py, pz = place(b)
        tile = hood3[px, py, pz]
        for d in range(3):
            xo[d, b] = tile[d : d + 1]
        sums = jnp.sum(
            qbuf[b] * jnp.where(xyz, tile + corner, 1.0), axis=1, keepdims=True
        )
        here = cell_ids == cell[b]
        return tuple(
            total + jnp.where(here, sums[d : d + 1], 0.0) for d, total in enumerate(totals)
        )

    zero = jnp.zeros((8, BLK), F32)
    moments = lax.fori_loop(0, NB, gather_moments, (zero, zero, zero, zero), unroll=4)
    for d in range(4):
        part0[d] = moments[d]

    stages = ((2, 4, part0, got0, 0), (0, 4, part1, got1, 3), (1, 8, part2, got2, 6))

    def spread(stage):
        axis, n, mine, got, base = stages[stage]
        return [
            pltpu.make_async_remote_copy(
                src_ref=mine,
                dst_ref=got.at[o - 1],
                send_sem=ms.at[base + o - 1],
                recv_sem=mr.at[base + o - 1],
                device_id=device(tuple(o if a == axis else 0 for a in range(3))),
                device_id_type=MESH,
            )
            for o in range(1, n)
        ]

    def collect(stage, copies):
        axis, n, mine, got, base = stages[stage]
        for copy in copies:
            copy.wait_recv()
        total = mine[...]
        for o in range(1, n):
            total = total + got[o - 1]
        return total

    spread0 = spread(0)
    for copy in spread0:
        copy.start()
    prepare_own(hood3)
    arrive(hood3, copies3, every)
    prepare(hood3)
    bond_kick(hood3, half_step)
    pair_kick(hood3, 0, 8)
    part1[...] = collect(0, spread0)
    spread1 = spread(1)
    for copy in spread1:
        copy.start()
    pair_kick(hood3, 8, 16)
    part2[...] = collect(1, spread1)
    spread2 = spread(2)
    for copy in spread2:
        copy.start()
    pair_kick(hood3, 16, 32)
    totals = collect(2, spread2)

    charge_sum = totals[3]
    places = [centre[d] for d in range(3)]
    dipole = [totals[d] - charge_sum * places[d] for d in range(3)]

    def finish(b, _):
        target = cell[b]
        away = [
            frac_s[d, target] * (1.0 * SIZES[d] * (SBX, SBY, SBZ)[d]) - places[d]
            for d in range(3)
        ]
        inverse = lax.rsqrt(
            away[0] * away[0] + away[1] * away[1] + away[2] * away[2] + soften * soften
        )
        cube = inverse * inverse * inverse
        fifth = cube * inverse * inverse
        along = dipole[0] * away[0] + dipole[1] * away[1] + dipole[2] * away[2]
        gain = charge_sum * cube + 3.0 * along * fifth
        field = [
            jnp.sum(gain * away[d] - dipole[d] * cube, axis=(0, 1), keepdims=True)
            for d in range(3)
        ]
        size = (outer_half * coulomb) * qbuf[b]
        v = vbuf[b]
        for d in range(3):
            vo[d, b] = v[d : d + 1] + size * field[d]
        return 0

    lax.fori_loop(0, NB, finish, 0, unroll=4)

    for copies in (copies0, copies1, copies2, copies3, spread0, spread1, spread2):
        for copy in copies:
            copy.wait_send()


def per_device(
    positions,
    velocities,
    strength,
    charge,
    bond_stiffness,
    bond_partner,
    pair_blocks,
    tile_count,
    block_cell,
    cell_frac,
    bond_force,
    pair_force,
    far_force,
):
    lines = lambda value, n: value.reshape(n, NB, 1, BLK)
    vmem = pl.BlockSpec(memory_space=pltpu.VMEM)
    smem = pl.BlockSpec(memory_space=pltpu.SMEM)
    hood = pltpu.VMEM((EX, EY, EZ, 4, BLK), F32)
    out = jax.ShapeDtypeStruct((3, NB, 1, BLK), F32)
    x, v = pl.pallas_call(
        kernel,
        out_shape=(out, out),
        in_specs=[vmem] * 10 + [smem] * 4,
        out_specs=(vmem, vmem),
        scratch_shapes=[
            hood,
            hood,
            hood,
            hood,
            pltpu.VMEM((NB, 4, BLK), F32),
            pltpu.VMEM((NB, 1, BLK), F32),
            pltpu.VMEM((NE, 32, BLK), BF16),
            pltpu.VMEM((NE, 16, BLK), BF16),
            pltpu.VMEM((NB, BLK, 32), BF16),
            pltpu.VMEM((3, 8, BLK), F32),
            pltpu.VMEM((4, 8, BLK), F32),
            pltpu.VMEM((4, 8, BLK), F32),
            pltpu.VMEM((4, 8, BLK), F32),
            pltpu.VMEM((3, 4, 8, BLK), F32),
            pltpu.VMEM((3, 4, 8, BLK), F32),
            pltpu.VMEM((7, 4, 8, BLK), F32),
            pltpu.SemaphoreType.DMA((4, 26)),
            pltpu.SemaphoreType.DMA((4, 26)),
            pltpu.SemaphoreType.DMA((13,)),
            pltpu.SemaphoreType.DMA((13,)),
        ],
        compiler_params=pltpu.CompilerParams(
            collective_id=0, has_side_effects=True, vmem_limit_bytes=48 * 1024 * 1024
        ),
        name="outer_step",
    )(
        lines(positions, 3),
        lines(velocities, 3),
        strength.reshape(NB, 1, BLK),
        charge.reshape(NB, 1, BLK),
        lines(bond_stiffness, 2),
        lines(bond_partner, 2),
        lines(bond_force, 3),
        lines(pair_force, 3),
        lines(far_force, 3),
        cell_frac,
        cell_frac,
        pair_blocks.reshape(NB, 8),
        block_cell.reshape(NB),
        tile_count.reshape(1),
    )
    return x.reshape(positions.shape), v.reshape(velocities.shape)


def solution(mesh):
    vector = P(None, "gx", "gy", "gz", None)
    scalar = P("gx", "gy", "gz", None)
    in_specs = (
        vector,
        vector,
        scalar,
        scalar,
        vector,
        vector,
        P("gx", "gy", "gz", None, None),
        P("gx", "gy", "gz"),
        scalar,
        P(),
        vector,
        vector,
        vector,
    )
    return jax.shard_map(
        per_device, mesh=mesh, in_specs=in_specs, out_specs=(vector, vector), check_vma=False
    )
```

```python
import math

import jax
import jax.numpy as jnp
from jax import lax
from jax.experimental import pallas as pl
from jax.experimental.pallas import tpu as pltpu
from jax.sharding import PartitionSpec as P

MESH = pl.DeviceIdType.MESH
SBX, SBY, SBZ = 4, 4, 2
BLK = 128
NB = SBX * SBY * SBZ
EX, EY, EZ = SBX + 2, SBY + 2, SBZ + 2
NE = EX * EY * EZ
CELLS = 1024
AXES = ("gx", "gy", "gz")

inner_step = 0.1
gauss_width = 0.25
pair_scale = 0.1
soften = 1.0
coulomb = 0.02
half_step = 0.5 * inner_step
outer_half = 2.0 * inner_step

rate = 1.0 / (2.0 * gauss_width * gauss_width)
bits = rate / math.log(2.0)
pair_factor = pair_scale / (gauss_width * gauss_width) * math.exp(-rate) / (bits * bits)

FACES = ((-1, 0, 0), (1, 0, 0), (0, -1, 0), (0, 1, 0), (0, 0, -1), (0, 0, 1))
AROUND = tuple(
    (dx, dy, dz)
    for dx in (-1, 0, 1)
    for dy in (-1, 0, 1)
    for dz in (-1, 0, 1)
    if (dx, dy, dz) != (0, 0, 0)
)
SIZES = (4, 8, 4)

F32 = jnp.float32
BF16 = jnp.bfloat16


def row_ids(n=4):
    return lax.broadcasted_iota(jnp.int32, (n, BLK), 0)


def rows4(a, b, c, d):
    r = row_ids()
    return jnp.where(r == 0, a, jnp.where(r == 1, b, jnp.where(r == 2, c, d)))


def place(b):
    return b // (SBY * SBZ) + 1, b // SBZ % SBY + 1, b % SBZ + 1


def lane_gather(values, lanes):
    numbers = lax.GatherDimensionNumbers(
        offset_dims=(),
        collapsed_slice_dims=(1,),
        start_index_map=(1,),
        operand_batching_dims=(0,),
        start_indices_batching_dims=(0,),
    )
    return lax.gather(
        values,
        lanes[..., None],
        numbers,
        slice_sizes=(1, 1),
        mode=lax.GatherScatterMode.PROMISE_IN_BOUNDS,
    )


def thirds(value):
    high = value.astype(BF16).astype(F32)
    rest = value - high
    middle = rest.astype(BF16).astype(F32)
    return high, middle, rest - middle


def send_box(step, inner, ghost):
    count = inner
    if step == 0:
        return 1, count
    if ghost:
        return (0 if step > 0 else count + 1), 1
    return (count if step > 0 else 1), 1


def box(direction, ghost):
    return [send_box(s, inner, ghost) for s, inner in zip(direction, (SBX, SBY, SBZ))]


def cut(where, lines=4):
    return tuple(pl.ds(start, size) for start, size in where) + (pl.ds(0, lines), slice(None))


def spots(where):
    (x, nx), (y, ny), (z, nz) = where
    return [(x + i, y + j, z + k) for i in range(nx) for j in range(ny) for k in range(nz)]


def flat(x, y, z):
    return (x * EY + y) * EZ + z


ORDER = sorted(AROUND, key=lambda d: (d[1] != 0, d[2] != 0, d))
SENDS = ORDER[::-1]
ORDER_Y = next(i for i, d in enumerate(ORDER) if d[1] != 0)


def kernel(
    pos_h,
    vel_h,
    stren_h,
    chg_h,
    stiff_h,
    part_h,
    bforce_h,
    pforce_h,
    fforce_h,
    frac_h,
    pairs_h,
    cell_h,
    count_h,
    xo,
    vo,
    pos,
    vel,
    stren,
    chg,
    stiff,
    part,
    bforce,
    pforce,
    fforce,
    frac,
    frac_s,
    pairs,
    cell,
    count,
    hood0,
    hood1,
    hood2,
    hood3,
    vbuf,
    qbuf,
    slots,
    aways,
    springs,
    near,
    pull,
    left,
    centre,
    part0,
    part1,
    part2,
    got0,
    got1,
    got2,
    ins,
    hs,
    hr,
    gs,
    gr,
    ms,
    mr,
):
    me = tuple(lax.axis_index(a) for a in AXES)

    def device(shift):
        return tuple(lax.rem(m + (s + n), n) for m, s, n in zip(me, shift, SIZES))

    barrier = pltpu.get_barrier_semaphore()
    peers = set(AROUND)
    for axis, n in ((2, 4), (0, 4), (1, 8)):
        for o in range(2, n - 1):
            peers.add(tuple(o if a == axis else 0 for a in range(3)))
    peers = sorted(peers)
    for shift in peers:
        pl.semaphore_signal(barrier, inc=1, device_id=device(shift), device_id_type=MESH)

    fetches = [
        pltpu.make_async_copy(source, target, ins.at[i])
        for i, (source, target) in enumerate(
            (
                (count_h, count),
                (pos_h, pos),
                (vel_h, vel),
                (fforce_h, fforce),
                (pforce_h, pforce),
                (bforce_h, bforce),
                (stren_h, stren),
                (part_h, part),
                (stiff_h, stiff),
                (chg_h, chg),
                (pairs_h, pairs),
                (cell_h, cell),
                (frac_h, frac),
                (frac_h, frac_s),
            )
        )
    ]
    for copy in fetches:
        copy.start()

    rows = row_ids()
    xyz = rows < 3
    lanes = lax.broadcasted_iota(jnp.int32, (1, BLK), 1)
    rows8 = row_ids(8)
    upper = rows8 < 4

    def halo(hood, which, directions, lines):
        return {
            d: pltpu.make_async_remote_copy(
                src_ref=hood.at[cut(box(d, False), lines)],
                dst_ref=hood.at[cut(box(d, True), lines)],
                send_sem=hs.at[which, AROUND.index(d)],
                recv_sem=hr.at[which, AROUND.index(d)],
                device_id=device(d),
                device_id_type=MESH,
            )
            for d in directions
        }

    def launch(copies):
        for d in SENDS:
            if d in copies:
                copies[d].start()

    def shift_of(d):
        return rows4(-SBX * d[0] * 1.0, -SBY * d[1] * 1.0, -SBZ * d[2] * 1.0, 0.0)

    def begin(b, _):
        px, py, pz = place(b)
        live = jnp.where(b * BLK + lanes < count[0], 1.0, 0.0)
        x = rows4(pos[0, b], pos[1, b], pos[2, b], stren[b] * live)
        v = [
            vel[d, b]
            + outer_half * fforce[d, b]
            + inner_step * pforce[d, b]
            + half_step * bforce[d, b]
            for d in range(3)
        ]
        v = rows4(v[0], v[1], v[2], 0.0)
        vbuf[b] = v
        hood0[px, py, pz] = x + inner_step * v
        return 0

    for copy in fetches[:7]:
        copy.wait()
    lax.fori_loop(0, NB, begin, 0, unroll=4)
    pl.semaphore_wait(barrier, len(peers))
    copies0 = halo(hood0, 0, FACES, 3)
    launch(copies0)

    for copy in fetches[7:]:
        copy.wait()

    def bonds(b, _):
        px, py, pz = place(b)
        live = jnp.where(b * BLK + lanes < count[0], 1.0, 0.0)
        qbuf[b] = chg[b] * live
        columns = jnp.where(upper, part[0, b], part[1, b])
        slots[b] = columns & (BLK - 1)
        aways[b] = jnp.where((rows8 & 3) < 3, (columns >> 7) - flat(px, py, pz), NE)
        spring = jnp.where(upper, stiff[0, b], stiff[1, b])
        springs[b] = jnp.where((rows8 & 3) < 3, spring, 0.0)
        return 0

    lax.fori_loop(0, NB, bonds, 0, unroll=4)
    for d in range(3):
        for k in range(8):
            centre[d, k : k + 1, :] = frac[d : d + 1, k * BLK : (k + 1) * BLK] * (
                1.0 * SIZES[d] * (SBX, SBY, SBZ)[d]
            )

    def pick(tile, b, d):
        twice = jnp.concatenate([tile, tile], axis=0)
        offset = (d[0] * EY + d[1]) * EZ + d[2]
        return twice, aways[b] == offset, lane_gather(twice, slots[b])

    def fold(value):
        return value[0:4] + value[4:8]

    def bond_inside(hood, size):
        for b in range(NB):
            p = tuple(int(i) for i in place(b))
            own, hit, other = pick(hood[p], b, (0, 0, 0))
            other = jnp.where(hit, other, 0.0)
            for d in FACES:
                q = tuple(i + j for i, j in zip(p, d))
                if all(1 <= i <= n for i, n in zip(q, (SBX, SBY, SBZ))):
                    _, hit, value = pick(hood[q], b, d)
                    other = jnp.where(hit, value, other)
            vbuf[b] = vbuf[b] + size * fold(springs[b] * (other - own))

    def bond_face(hood, size, d):
        shift = shift_of(d)
        for q in spots(box(d, True)):
            e = tuple(-i for i in d)
            p = tuple(i + j for i, j in zip(q, d))
            b = ((p[0] - 1) * SBY + p[1] - 1) * SBZ + p[2] - 1
            _, hit, value = pick(hood[q] + shift, b, e)
            vbuf[b] = vbuf[b] + size * fold(jnp.where(hit, springs[b] * value, 0.0))

    def drift(hood, after):
        for b in range(NB):
            p = tuple(int(i) for i in place(b))
            after[p] = hood[p] + inner_step * vbuf[b]

    middle = rows4(0.5 * SBX, 0.5 * SBY, 0.5 * SBZ, 0.0)
    ones = jnp.where(xyz, 1.0, 0.0)
    blank = jnp.zeros((4, BLK), F32)

    def square_sum(z):
        return jnp.sum(jnp.where(xyz, z * z, 0.0), axis=0, keepdims=True)

    def prepare(e, z, a):
        high, mid, low = thirds(jnp.where(xyz, z, -bits * square_sum(z)))
        near[e] = jnp.concatenate(
            [high, mid, low, high, mid, high, ones, blank], axis=0
        ).astype(BF16)
        high, mid, low = thirds(jnp.where(xyz, z * a, a))
        pull[e] = jnp.concatenate([high, mid, low, blank], axis=0).astype(BF16)

    def prepare_ghosts(hood, d):
        shift = shift_of(d) - middle
        for q in spots(box(d, True)):
            prepare(flat(*q), hood[q] + shift, hood1[q][3:4])

    def prepare_own(hood):
        def body(b, _):
            px, py, pz = place(b)
            tile = hood[px, py, pz]
            z = tile - middle
            prepare(flat(px, py, pz), z, tile[3:4])
            high, mid, low = thirds(jnp.where(xyz, (2.0 * bits) * z, 1.0))
            ph, pm, pw = thirds(bits - bits * square_sum(z))
            stack = jnp.concatenate(
                [high, high, high, mid, mid, low, rows4(ph, pm, pw, 0.0), blank], axis=0
            )
            left[b] = stack.T.astype(BF16)
            return 0

        lax.fori_loop(0, NB, body, 0, unroll=4)

    def pair(hood, c, p):
        listed = [pairs[k, c] for k in range(8)]
        t = jnp.dot(
            left[c],
            jnp.concatenate([near[e] for e in listed], axis=1),
            preferred_element_type=F32,
        )
        r = jnp.maximum(t, 0.0)
        w = jnp.exp2(t) * (r * r)
        high = w.astype(BF16)
        low = (w - high.astype(F32)).astype(BF16)
        y = jnp.concatenate([pull[e] for e in listed], axis=1)
        over = (((1,), (1,)), ((), ()))
        acc = lax.dot_general(high, y, over, preferred_element_type=F32)
        acc = acc + lax.dot_general(low, y, over, preferred_element_type=F32)
        s = acc.T
        f = s[0:4] + s[4:8] + s[8:12]
        tile = hood[p]
        z = tile - middle
        force = (pair_factor * tile[3:4]) * (z * f[3:4] - f)
        return tile, jnp.where(xyz, force, 0.0)

    def pair_groups(hood, body):
        def group(g, _):
            by = jnp.where(g == 0, 0, jnp.where(g == 1, SBY - 1, g - 1))
            for bx in range(SBX):
                for bz in range(SBZ):
                    c = (bx * SBY + by) * SBZ + bz
                    p = (bx + 1, by + 1, bz + 1)
                    body(c, p, *pair(hood, c, p))
            return by

        return group

    bond_inside(hood0, inner_step)
    for d in ORDER:
        if d in copies0:
            copies0[d].wait_recv()
            bond_face(hood0, inner_step, d)
    drift(hood0, hood1)
    copies1 = halo(hood1, 1, AROUND, 4)
    launch(copies1)
    prepare_own(hood1)
    bond_inside(hood1, inner_step)
    for d in ORDER:
        copies1[d].wait_recv()
        prepare_ghosts(hood1, d)
        if d in FACES:
            bond_face(hood1, inner_step, d)

    def pieces(by, g):
        found = []
        for i, d in enumerate(FACES):
            if d[1] == 0:
                src, dst = box(d, False), box(d, True)
                src[1] = dst[1] = (by + 1, 1)
                found.append(
                    pltpu.make_async_remote_copy(
                        src_ref=hood2.at[cut(src, 3)],
                        dst_ref=hood2.at[cut(dst, 3)],
                        send_sem=gs.at[g, i],
                        recv_sem=gr.at[g, i],
                        device_id=device(d),
                        device_id_type=MESH,
                    )
                )
        return found

    copies2 = halo(hood2, 2, ((0, -1, 0), (0, 1, 0)), 3)

    def kick_drift(c, p, tile, force):
        v = vbuf[c] + (2.0 * inner_step) * force
        vbuf[c] = v
        hood2[p] = tile + inner_step * v

    first = pair_groups(hood1, kick_drift)

    def first_group(g, _):
        by = first(g, 0)

        @pl.when(g == 0)
        def _():
            copies2[(0, -1, 0)].start()

        @pl.when(g == 1)
        def _():
            copies2[(0, 1, 0)].start()

        for copy in pieces(by, g):
            copy.start()
        return 0

    lax.fori_loop(0, SBY, first_group, 0)
    parts2 = [pieces(by, g) for g, by in enumerate((0, SBY - 1, 1, 2))]
    bond_inside(hood2, inner_step)
    for i, d in enumerate([d for d in FACES if d[1] == 0]):
        for group in parts2:
            group[i].wait_recv()
        bond_face(hood2, inner_step, d)
    for d in copies2:
        copies2[d].wait_recv()
        bond_face(hood2, inner_step, d)
    drift(hood2, hood3)
    copies3 = halo(hood3, 3, AROUND, 3)
    launch(copies3)

    cell_ids = lax.broadcasted_iota(jnp.int32, (8, BLK), 0) * BLK + lax.broadcasted_iota(
        jnp.int32, (8, BLK), 1
    )
    corner = rows4(
        (me[0] * SBX).astype(F32), (me[1] * SBY).astype(F32), (me[2] * SBZ).astype(F32), 0.0
    )

    def gather_moments(b, totals):
        px, py, pz = place(b)
        tile = hood3[px, py, pz]
        for d in range(3):
            xo[d, b] = tile[d : d + 1]
        sums = jnp.sum(
            qbuf[b] * jnp.where(xyz, tile + corner, 1.0), axis=1, keepdims=True
        )
        here = cell_ids == cell[b]
        return tuple(
            total + jnp.where(here, sums[d : d + 1], 0.0) for d, total in enumerate(totals)
        )

    zero = jnp.zeros((8, BLK), F32)
    moments = lax.fori_loop(0, NB, gather_moments, (zero, zero, zero, zero), unroll=4)
    for d in range(4):
        part0[d] = moments[d]

    stages = ((2, 4, part0, got0, 0), (0, 4, part1, got1, 3), (1, 8, part2, got2, 6))

    def spread(stage):
        axis, n, mine, got, base = stages[stage]
        return [
            pltpu.make_async_remote_copy(
                src_ref=mine,
                dst_ref=got.at[o - 1],
                send_sem=ms.at[base + o - 1],
                recv_sem=mr.at[base + o - 1],
                device_id=device(tuple(o if a == axis else 0 for a in range(3))),
                device_id_type=MESH,
            )
            for o in range(1, n)
        ]

    spreads = [spread(stage) for stage in range(3)]

    def send_moments(stage):
        for copy in spreads[stage]:
            copy.start()

    def collect(stage):
        axis, n, mine, got, base = stages[stage]
        for copy in spreads[stage]:
            copy.wait_recv()
        total = mine[...]
        for o in range(1, n):
            total = total + got[o - 1]
        return total

    send_moments(0)
    prepare_own(hood3)
    bond_inside(hood3, half_step)

    for d in ORDER:
        if d == ORDER[ORDER_Y]:
            part1[...] = collect(0)
            send_moments(1)
        copies3[d].wait_recv()
        prepare_ghosts(hood3, d)
        if d in FACES:
            bond_face(hood3, half_step, d)

    def kick(c, p, tile, force):
        vbuf[c] = vbuf[c] + inner_step * force

    second = pair_groups(hood3, kick)

    def second_group(g, _):
        second(g, 0)

        @pl.when(g == 0)
        def _():
            part2[...] = collect(1)
            send_moments(2)

        return 0

    lax.fori_loop(0, SBY, second_group, 0)
    totals = collect(2)

    charge_sum = totals[3]
    places = [centre[d] for d in range(3)]
    dipole = [totals[d] - charge_sum * places[d] for d in range(3)]

    def finish(b, _):
        target = cell[b]
        away = [
            frac_s[d, target] * (1.0 * SIZES[d] * (SBX, SBY, SBZ)[d]) - places[d]
            for d in range(3)
        ]
        inverse = lax.rsqrt(
            away[0] * away[0] + away[1] * away[1] + away[2] * away[2] + soften * soften
        )
        cube = inverse * inverse * inverse
        fifth = cube * inverse * inverse
        along = dipole[0] * away[0] + dipole[1] * away[1] + dipole[2] * away[2]
        gain = charge_sum * cube + 3.0 * along * fifth
        field = [
            jnp.sum(gain * away[d] - dipole[d] * cube, axis=(0, 1), keepdims=True)
            for d in range(3)
        ]
        size = (outer_half * coulomb) * qbuf[b]
        v = vbuf[b]
        for d in range(3):
            vo[d, b] = v[d : d + 1] + size * field[d]
        return 0

    lax.fori_loop(0, NB, finish, 0, unroll=4)

    sent = [copies[d] for copies in (copies0, copies1, copies2, copies3) for d in copies]
    for copies in parts2 + spreads:
        sent += copies
    for copy in sent:
        copy.wait_send()


def per_device(
    positions,
    velocities,
    strength,
    charge,
    bond_stiffness,
    bond_partner,
    pair_blocks,
    tile_count,
    block_cell,
    cell_frac,
    bond_force,
    pair_force,
    far_force,
):
    lines = lambda value, n: value.reshape(n, NB, 1, BLK)
    vmem = pl.BlockSpec(memory_space=pltpu.VMEM)
    anywhere = pl.BlockSpec(memory_space=pl.ANY)
    hood = pltpu.VMEM((EX, EY, EZ, 4, BLK), F32)
    line3 = pltpu.VMEM((3, NB, 1, BLK), F32)
    line2 = pltpu.VMEM((2, NB, 1, BLK), F32)
    line1 = pltpu.VMEM((NB, 1, BLK), F32)
    sums = pltpu.VMEM((4, 8, BLK), F32)
    out = jax.ShapeDtypeStruct((3, NB, 1, BLK), F32)
    x, v = pl.pallas_call(
        kernel,
        out_shape=(out, out),
        in_specs=[anywhere] * 13,
        out_specs=(vmem, vmem),
        scratch_shapes=[
            line3,
            line3,
            line1,
            line1,
            line2,
            pltpu.VMEM((2, NB, 1, BLK), jnp.int32),
            line3,
            line3,
            line3,
            pltpu.VMEM((3, CELLS), F32),
            pltpu.SMEM((3, CELLS), F32),
            pltpu.SMEM((8, NB), jnp.int32),
            pltpu.SMEM((NB,), jnp.int32),
            pltpu.SMEM((1,), jnp.int32),
            hood,
            hood,
            hood,
            hood,
            pltpu.VMEM((NB, 4, BLK), F32),
            line1,
            pltpu.VMEM((NB, 8, BLK), jnp.int32),
            pltpu.VMEM((NB, 8, BLK), jnp.int32),
            pltpu.VMEM((NB, 8, BLK), F32),
            pltpu.VMEM((NE, 32, BLK), BF16),
            pltpu.VMEM((NE, 16, BLK), BF16),
            pltpu.VMEM((NB, BLK, 32), BF16),
            pltpu.VMEM((3, 8, BLK), F32),
            sums,
            sums,
            sums,
            pltpu.VMEM((3, 4, 8, BLK), F32),
            pltpu.VMEM((3, 4, 8, BLK), F32),
            pltpu.VMEM((7, 4, 8, BLK), F32),
            pltpu.SemaphoreType.DMA((14,)),
            pltpu.SemaphoreType.DMA((4, 26)),
            pltpu.SemaphoreType.DMA((4, 26)),
            pltpu.SemaphoreType.DMA((4, 6)),
            pltpu.SemaphoreType.DMA((4, 6)),
            pltpu.SemaphoreType.DMA((13,)),
            pltpu.SemaphoreType.DMA((13,)),
        ],
        compiler_params=pltpu.CompilerParams(
            collective_id=0, has_side_effects=True, vmem_limit_bytes=60 * 1024 * 1024
        ),
        name="outer_step",
    )(
        lines(positions, 3),
        lines(velocities, 3),
        strength.reshape(NB, 1, BLK),
        charge.reshape(NB, 1, BLK),
        lines(bond_stiffness, 2),
        lines(bond_partner, 2),
        lines(bond_force, 3),
        lines(pair_force, 3),
        lines(far_force, 3),
        cell_frac,
        pair_blocks.reshape(NB, 8).T,
        block_cell.reshape(NB),
        tile_count.reshape(1),
    )
    return x.reshape(positions.shape), v.reshape(velocities.shape)


def solution(mesh):
    vector = P(None, "gx", "gy", "gz", None)
    scalar = P("gx", "gy", "gz", None)
    in_specs = (
        vector,
        vector,
        scalar,
        scalar,
        vector,
        vector,
        P("gx", "gy", "gz", None, None),
        P("gx", "gy", "gz"),
        scalar,
        P(),
        vector,
        vector,
        vector,
    )
    return jax.shard_map(
        per_device, mesh=mesh, in_specs=in_specs, out_specs=(vector, vector), check_vma=False
    )
```

```python
import math

import jax
import jax.numpy as jnp
from jax import lax
from jax.experimental import pallas as pl
from jax.experimental.pallas import tpu as pltpu
from jax.sharding import PartitionSpec as P

MESH = pl.DeviceIdType.MESH
SBX, SBY, SBZ = 4, 4, 2
BLK = 128
NB = SBX * SBY * SBZ
EX, EY, EZ = SBX + 2, SBY + 2, SBZ + 2
NE = EX * EY * EZ
CELLS = 1024
AXES = ("gx", "gy", "gz")

inner_step = 0.1
gauss_width = 0.25
pair_scale = 0.1
soften = 1.0
coulomb = 0.02
half_step = 0.5 * inner_step
outer_half = 2.0 * inner_step

rate = 1.0 / (2.0 * gauss_width * gauss_width)
bits = rate / math.log(2.0)
pair_factor = pair_scale / (gauss_width * gauss_width) * math.exp(-rate) / (bits * bits)

FACES = ((-1, 0, 0), (1, 0, 0), (0, -1, 0), (0, 1, 0), (0, 0, -1), (0, 0, 1))
AROUND = tuple(
    (dx, dy, dz)
    for dx in (-1, 0, 1)
    for dy in (-1, 0, 1)
    for dz in (-1, 0, 1)
    if (dx, dy, dz) != (0, 0, 0)
)
SIZES = (4, 8, 4)

F32 = jnp.float32
BF16 = jnp.bfloat16


def row_ids(n=4):
    return lax.broadcasted_iota(jnp.int32, (n, BLK), 0)


def rows4(a, b, c, d):
    r = row_ids()
    return jnp.where(r == 0, a, jnp.where(r == 1, b, jnp.where(r == 2, c, d)))


def place(b):
    return b // (SBY * SBZ) + 1, b // SBZ % SBY + 1, b % SBZ + 1


def lane_gather(values, lanes):
    numbers = lax.GatherDimensionNumbers(
        offset_dims=(),
        collapsed_slice_dims=(1,),
        start_index_map=(1,),
        operand_batching_dims=(0,),
        start_indices_batching_dims=(0,),
    )
    return lax.gather(
        values,
        lanes[..., None],
        numbers,
        slice_sizes=(1, 1),
        mode=lax.GatherScatterMode.PROMISE_IN_BOUNDS,
    )


def thirds(value):
    high = value.astype(BF16).astype(F32)
    rest = value - high
    middle = rest.astype(BF16).astype(F32)
    return high, middle, rest - middle


def send_box(step, inner, ghost):
    count = inner
    if step == 0:
        return 1, count
    if ghost:
        return (0 if step > 0 else count + 1), 1
    return (count if step > 0 else 1), 1


def box(direction, ghost):
    return [send_box(s, inner, ghost) for s, inner in zip(direction, (SBX, SBY, SBZ))]


def part_box(direction, ghost, rows):
    where = box(direction, ghost)
    if direction[1] == 0:
        where[1] = (rows[0] + 1, rows[1])
    return where


def cut(where, lines=4):
    return tuple(pl.ds(start, size) for start, size in where) + (pl.ds(0, lines), slice(None))


def spots(where):
    (x, nx), (y, ny), (z, nz) = where
    return [(x + i, y + j, z + k) for i in range(nx) for j in range(ny) for k in range(nz)]


def flat(x, y, z):
    return (x * EY + y) * EZ + z


ORDER = sorted(AROUND, key=lambda d: (d[1] != 0, d[2] != 0, d))
SENDS = ORDER[::-1]
ORDER_Y = next(i for i, d in enumerate(ORDER) if d[1] != 0)


def kernel(
    pos_h,
    vel_h,
    stren_h,
    chg_h,
    stiff_h,
    part_h,
    bforce_h,
    pforce_h,
    fforce_h,
    frac_h,
    pairs_h,
    cell_h,
    count_h,
    oo,
    pos,
    vel,
    stren,
    chg,
    stiff,
    part,
    bforce,
    pforce,
    fforce,
    frac,
    frac_s,
    pairs,
    cell,
    count,
    hood0,
    hood1,
    hood2,
    hood3,
    vbuf,
    qbuf,
    slots,
    aways,
    springs,
    near,
    pull,
    left,
    centre,
    part0,
    part1,
    part2,
    got0,
    got1,
    got2,
    ins,
    hs,
    hr,
    gs,
    gr,
    rs,
    rr,
    ms,
    mr,
):
    me = tuple(lax.axis_index(a) for a in AXES)

    def device(shift):
        return tuple(lax.rem(m + (s + n), n) for m, s, n in zip(me, shift, SIZES))

    barrier = pltpu.get_barrier_semaphore()
    peers = set(AROUND)
    for axis, n in ((2, 4), (0, 4), (1, 8)):
        for o in range(2, n - 1):
            peers.add(tuple(o if a == axis else 0 for a in range(3)))
    peers = sorted(peers)
    for shift in peers:
        pl.semaphore_signal(barrier, inc=1, device_id=device(shift), device_id_type=MESH)

    fetches = [
        pltpu.make_async_copy(source, target, ins.at[i])
        for i, (source, target) in enumerate(
            (
                (count_h, count),
                (pos_h, pos),
                (vel_h, vel),
                (fforce_h, fforce),
                (pforce_h, pforce),
                (bforce_h, bforce),
                (stren_h, stren),
                (part_h, part),
                (stiff_h, stiff),
                (chg_h, chg),
                (pairs_h, pairs),
                (cell_h, cell),
                (frac_h, frac),
                (frac_h, frac_s),
            )
        )
    ]
    for copy in fetches:
        copy.start()

    rows = row_ids()
    xyz = rows < 3
    lanes = lax.broadcasted_iota(jnp.int32, (1, BLK), 1)
    rows8 = row_ids(8)
    upper = rows8 < 4

    def halo(hood, which, directions, lines):
        return {
            d: pltpu.make_async_remote_copy(
                src_ref=hood.at[cut(box(d, False), lines)],
                dst_ref=hood.at[cut(box(d, True), lines)],
                send_sem=hs.at[which, AROUND.index(d)],
                recv_sem=hr.at[which, AROUND.index(d)],
                device_id=device(d),
                device_id_type=MESH,
            )
            for d in directions
        }

    def launch(copies):
        for d in SENDS:
            if d in copies:
                copies[d].start()

    def shift_of(d):
        return rows4(-SBX * d[0] * 1.0, -SBY * d[1] * 1.0, -SBZ * d[2] * 1.0, 0.0)

    def begin(b, _):
        px, py, pz = place(b)
        live = jnp.where(b * BLK + lanes < count[0], 1.0, 0.0)
        x = rows4(pos[0, b], pos[1, b], pos[2, b], stren[b] * live)
        v = [
            vel[d, b]
            + outer_half * fforce[d, b]
            + inner_step * pforce[d, b]
            + half_step * bforce[d, b]
            for d in range(3)
        ]
        v = rows4(v[0], v[1], v[2], 0.0)
        vbuf[b] = v
        hood0[px, py, pz] = x + inner_step * v
        return 0

    for copy in fetches[:7]:
        copy.wait()
    lax.fori_loop(0, NB, begin, 0, unroll=4)
    pl.semaphore_wait(barrier, len(peers))
    copies0 = halo(hood0, 0, FACES, 3)
    launch(copies0)

    for copy in fetches[7:]:
        copy.wait()

    def bonds(b, _):
        px, py, pz = place(b)
        live = jnp.where(b * BLK + lanes < count[0], 1.0, 0.0)
        qbuf[b] = chg[b] * live
        columns = jnp.where(upper, part[0, b], part[1, b])
        slots[b] = columns & (BLK - 1)
        aways[b] = jnp.where((rows8 & 3) < 3, (columns >> 7) - flat(px, py, pz), NE)
        spring = jnp.where(upper, stiff[0, b], stiff[1, b])
        springs[b] = jnp.where((rows8 & 3) < 3, spring, 0.0)
        return 0

    lax.fori_loop(0, NB, bonds, 0, unroll=4)
    for d in range(3):
        for k in range(8):
            centre[d, k : k + 1, :] = frac[d : d + 1, k * BLK : (k + 1) * BLK] * (
                1.0 * SIZES[d] * (SBX, SBY, SBZ)[d]
            )

    def pick(tile, b, d):
        twice = jnp.concatenate([tile, tile], axis=0)
        offset = (d[0] * EY + d[1]) * EZ + d[2]
        return twice, aways[b] == offset, lane_gather(twice, slots[b])

    def fold(value):
        return value[0:4] + value[4:8]

    def bond_inside(hood, size):
        for b in range(NB):
            p = tuple(int(i) for i in place(b))
            own, hit, other = pick(hood[p], b, (0, 0, 0))
            other = jnp.where(hit, other, 0.0)
            for d in FACES:
                q = tuple(i + j for i, j in zip(p, d))
                if all(1 <= i <= n for i, n in zip(q, (SBX, SBY, SBZ))):
                    _, hit, value = pick(hood[q], b, d)
                    other = jnp.where(hit, value, other)
            vbuf[b] = vbuf[b] + size * fold(springs[b] * (other - own))

    def bond_face(hood, size, d, rows=(0, SBY)):
        shift = shift_of(d)
        for q in spots(part_box(d, True, rows)):
            e = tuple(-i for i in d)
            p = tuple(i + j for i, j in zip(q, d))
            b = ((p[0] - 1) * SBY + p[1] - 1) * SBZ + p[2] - 1
            _, hit, value = pick(hood[q] + shift, b, e)
            vbuf[b] = vbuf[b] + size * fold(jnp.where(hit, springs[b] * value, 0.0))

    def drift(hood, after, row=None):
        for b in range(NB):
            p = tuple(int(i) for i in place(b))
            if row is None or p[1] == row + 1:
                after[p] = hood[p] + inner_step * vbuf[b]

    middle = rows4(0.5 * SBX, 0.5 * SBY, 0.5 * SBZ, 0.0)
    ones = jnp.where(xyz, 1.0, 0.0)
    blank = jnp.zeros((4, BLK), F32)

    def square_sum(z):
        return jnp.sum(jnp.where(xyz, z * z, 0.0), axis=0, keepdims=True)

    def prepare(e, z, a):
        high, mid, low = thirds(jnp.where(xyz, z, -bits * square_sum(z)))
        near[e] = jnp.concatenate(
            [high, mid, low, high, mid, high, ones, blank], axis=0
        ).astype(BF16)
        high, mid, low = thirds(jnp.where(xyz, z * a, a))
        pull[e] = jnp.concatenate([high, mid, low, blank], axis=0).astype(BF16)

    def prepare_ghosts(hood, d, rows=(0, SBY)):
        shift = shift_of(d) - middle
        for q in spots(part_box(d, True, rows)):
            prepare(flat(*q), hood[q] + shift, hood1[q][3:4])

    def prepare_own(hood):
        def body(b, _):
            px, py, pz = place(b)
            tile = hood[px, py, pz]
            z = tile - middle
            prepare(flat(px, py, pz), z, tile[3:4])
            high, mid, low = thirds(jnp.where(xyz, (2.0 * bits) * z, 1.0))
            ph, pm, pw = thirds(bits - bits * square_sum(z))
            stack = jnp.concatenate(
                [high, high, high, mid, mid, low, rows4(ph, pm, pw, 0.0), blank], axis=0
            )
            left[b] = stack.T.astype(BF16)
            return 0

        lax.fori_loop(0, NB, body, 0, unroll=4)

    def pair(hood, c, p):
        listed = [pairs[k, c] for k in range(8)]
        t = jnp.dot(
            left[c],
            jnp.concatenate([near[e] for e in listed], axis=1),
            preferred_element_type=F32,
        )
        r = jnp.maximum(t, 0.0)
        w = jnp.exp2(t) * (r * r)
        high = w.astype(BF16)
        low = (w - high.astype(F32)).astype(BF16)
        y = jnp.concatenate([pull[e] for e in listed], axis=1)
        over = (((1,), (1,)), ((), ()))
        acc = lax.dot_general(high, y, over, preferred_element_type=F32)
        acc = acc + lax.dot_general(low, y, over, preferred_element_type=F32)
        s = acc.T
        f = s[0:4] + s[4:8] + s[8:12]
        tile = hood[p]
        z = tile - middle
        force = (pair_factor * tile[3:4]) * (z * f[3:4] - f)
        return tile, jnp.where(xyz, force, 0.0)

    def pair_row(hood, by, body):
        for bx in range(SBX):
            for bz in range(SBZ):
                c = (bx * SBY + by) * SBZ + bz
                p = (bx + 1, by + 1, bz + 1)
                body(c, p, *pair(hood, c, p))

    bond_inside(hood0, inner_step)
    for d in ORDER:
        if d in copies0:
            copies0[d].wait_recv()
            bond_face(hood0, inner_step, d)
    drift(hood0, hood1)
    copies1 = halo(hood1, 1, AROUND, 4)
    launch(copies1)
    prepare_own(hood1)
    bond_inside(hood1, inner_step)
    def take1(d):
        copies1[d].wait_recv()
        prepare_ghosts(hood1, d)
        if d in FACES:
            bond_face(hood1, inner_step, d)

    def row_copies(hood, directions, by, sends, recvs):
        rows = (by, 1)
        return {
            d: pltpu.make_async_remote_copy(
                src_ref=hood.at[cut(part_box(d, False, rows), 3)],
                dst_ref=hood.at[cut(part_box(d, True, rows), 3)],
                send_sem=sends.at[by, i],
                recv_sem=recvs.at[by, i],
                device_id=device(d),
                device_id_type=MESH,
            )
            for i, d in enumerate(directions)
        }

    flat_faces = [d for d in FACES if d[1] == 0]
    copies2 = halo(hood2, 2, ((0, -1, 0), (0, 1, 0)), 3)
    parts2 = [row_copies(hood2, flat_faces, by, gs, gr) for by in range(SBY)]

    def kick_drift(c, p, tile, force):
        v = vbuf[c] + (2.0 * inner_step) * force
        vbuf[c] = v
        hood2[p] = tile + inner_step * v

    for d in ORDER[:ORDER_Y]:
        take1(d)

    def first_row(g, _):
        by = jnp.where(g == 0, 1, jnp.where(g == 1, 0, jnp.where(g == 2, SBY - 1, 2)))
        pair_row(hood1, by, kick_drift)

        @pl.when(g == 0)
        def _():
            for d in ORDER[ORDER_Y:]:
                take1(d)

        @pl.when(g == 1)
        def _():
            copies2[(0, -1, 0)].start()

        @pl.when(g == 2)
        def _():
            copies2[(0, 1, 0)].start()

        for copy in row_copies(hood2, flat_faces, by, gs, gr).values():
            copy.start()
        return 0

    lax.fori_loop(0, SBY, first_row, 0)
    copies3 = halo(hood3, 3, [d for d in AROUND if d[1] != 0], 3)
    flat_around = [d for d in AROUND if d[1] == 0]
    parts3 = [row_copies(hood3, flat_around, by, rs, rr) for by in range(SBY)]
    bond_inside(hood2, inner_step)
    for by in (1, SBY - 1, 0, 2):
        for d in flat_faces:
            parts2[by][d].wait_recv()
            bond_face(hood2, inner_step, d, (by, 1))
        if by in (0, SBY - 1):
            d = (0, 1, 0) if by == 0 else (0, -1, 0)
            copies2[d].wait_recv()
            bond_face(hood2, inner_step, d)
        drift(hood2, hood3, by)
        if by in (0, SBY - 1):
            launch({d: copies3[d] for d in copies3 if d[1] == (-1 if by == 0 else 1)})
        launch(parts3[by])
    cell_ids = lax.broadcasted_iota(jnp.int32, (8, BLK), 0) * BLK + lax.broadcasted_iota(
        jnp.int32, (8, BLK), 1
    )
    corner = rows4(
        (me[0] * SBX).astype(F32), (me[1] * SBY).astype(F32), (me[2] * SBZ).astype(F32), 0.0
    )

    def gather_moments(b, totals):
        px, py, pz = place(b)
        tile = hood3[px, py, pz]
        for d in range(3):
            oo[d, b] = tile[d : d + 1]
        sums = jnp.sum(
            qbuf[b] * jnp.where(xyz, tile + corner, 1.0), axis=1, keepdims=True
        )
        here = cell_ids == cell[b]
        return tuple(
            total + jnp.where(here, sums[d : d + 1], 0.0) for d, total in enumerate(totals)
        )

    zero = jnp.zeros((8, BLK), F32)
    moments = lax.fori_loop(0, NB, gather_moments, (zero, zero, zero, zero), unroll=4)
    for d in range(4):
        part0[d] = moments[d]

    stages = ((2, 4, part0, got0, 0), (0, 4, part1, got1, 3), (1, 8, part2, got2, 6))

    def spread(stage):
        axis, n, mine, got, base = stages[stage]
        return [
            pltpu.make_async_remote_copy(
                src_ref=mine,
                dst_ref=got.at[o - 1],
                send_sem=ms.at[base + o - 1],
                recv_sem=mr.at[base + o - 1],
                device_id=device(tuple(o if a == axis else 0 for a in range(3))),
                device_id_type=MESH,
            )
            for o in range(1, n)
        ]

    spreads = [spread(stage) for stage in range(3)]

    def send_moments(stage):
        for copy in spreads[stage]:
            copy.start()

    def collect(stage):
        axis, n, mine, got, base = stages[stage]
        for copy in spreads[stage]:
            copy.wait_recv()
        total = mine[...]
        for o in range(1, n):
            total = total + got[o - 1]
        return total

    send_moments(0)
    prepare_own(hood3)
    bond_inside(hood3, half_step)

    def take3(copies, d, rows=(0, SBY)):
        copies[d].wait_recv()
        prepare_ghosts(hood3, d, rows)
        if d in FACES:
            bond_face(hood3, half_step, d, rows)

    def kick(c, p, tile, force):
        vbuf[c] = vbuf[c] + inner_step * force

    for by in (1, SBY - 1, 0):
        for d in flat_around:
            take3(parts3[by], d, (by, 1))
    for d in ORDER[ORDER_Y:]:
        if d[1] > 0:
            take3(copies3, d)

    def second_row(by, _):
        pair_row(hood3, by, kick)

        @pl.when(by == 0)
        def _():
            part1[...] = collect(0)
            send_moments(1)
            for d in flat_around:
                take3(parts3[2], d, (2, 1))
            for d in ORDER[ORDER_Y:]:
                if d[1] < 0:
                    take3(copies3, d)

        @pl.when(by == 1)
        def _():
            part2[...] = collect(1)
            send_moments(2)

        return 0

    lax.fori_loop(0, SBY, second_row, 0)
    totals = collect(2)

    charge_sum = totals[3]
    places = [centre[d] for d in range(3)]
    dipole = [totals[d] - charge_sum * places[d] for d in range(3)]

    def finish(b, _):
        target = cell[b]
        away = [
            frac_s[d, target] * (1.0 * SIZES[d] * (SBX, SBY, SBZ)[d]) - places[d]
            for d in range(3)
        ]
        inverse = lax.rsqrt(
            away[0] * away[0] + away[1] * away[1] + away[2] * away[2] + soften * soften
        )
        cube = inverse * inverse * inverse
        fifth = cube * inverse * inverse
        along = dipole[0] * away[0] + dipole[1] * away[1] + dipole[2] * away[2]
        gain = charge_sum * cube + 3.0 * along * fifth
        field = [
            jnp.sum(gain * away[d] - dipole[d] * cube, axis=(0, 1), keepdims=True)
            for d in range(3)
        ]
        size = (outer_half * coulomb) * qbuf[b]
        v = vbuf[b]
        for d in range(3):
            oo[3 + d, b] = v[d : d + 1] + size * field[d]
        return 0

    lax.fori_loop(0, NB, finish, 0, unroll=4)

    sent = [copies[d] for copies in (copies0, copies1, copies2, copies3) for d in copies]
    for copies in parts2 + parts3:
        sent += copies.values()
    for copies in spreads:
        sent += copies
    for copy in sent:
        copy.wait_send()


def per_device(
    positions,
    velocities,
    strength,
    charge,
    bond_stiffness,
    bond_partner,
    pair_blocks,
    tile_count,
    block_cell,
    cell_frac,
    bond_force,
    pair_force,
    far_force,
):
    lines = lambda value, n: value.reshape(n, NB, 1, BLK)
    vmem = pl.BlockSpec(memory_space=pltpu.VMEM)
    anywhere = pl.BlockSpec(memory_space=pl.ANY)
    hood = pltpu.VMEM((EX, EY, EZ, 4, BLK), F32)
    line3 = pltpu.VMEM((3, NB, 1, BLK), F32)
    line2 = pltpu.VMEM((2, NB, 1, BLK), F32)
    line1 = pltpu.VMEM((NB, 1, BLK), F32)
    sums = pltpu.VMEM((4, 8, BLK), F32)
    out = jax.ShapeDtypeStruct((3, NB, 1, BLK), F32)
    xv = pl.pallas_call(
        kernel,
        out_shape=jax.ShapeDtypeStruct((6, NB, 1, BLK), F32),
        in_specs=[anywhere] * 13,
        out_specs=vmem,
        scratch_shapes=[
            line3,
            line3,
            line1,
            line1,
            line2,
            pltpu.VMEM((2, NB, 1, BLK), jnp.int32),
            line3,
            line3,
            line3,
            pltpu.VMEM((3, CELLS), F32),
            pltpu.SMEM((3, CELLS), F32),
            pltpu.SMEM((8, NB), jnp.int32),
            pltpu.SMEM((NB,), jnp.int32),
            pltpu.SMEM((1,), jnp.int32),
            hood,
            hood,
            hood,
            hood,
            pltpu.VMEM((NB, 4, BLK), F32),
            line1,
            pltpu.VMEM((NB, 8, BLK), jnp.int32),
            pltpu.VMEM((NB, 8, BLK), jnp.int32),
            pltpu.VMEM((NB, 8, BLK), F32),
            pltpu.VMEM((NE, 32, BLK), BF16),
            pltpu.VMEM((NE, 16, BLK), BF16),
            pltpu.VMEM((NB, BLK, 32), BF16),
            pltpu.VMEM((3, 8, BLK), F32),
            sums,
            sums,
            sums,
            pltpu.VMEM((3, 4, 8, BLK), F32),
            pltpu.VMEM((3, 4, 8, BLK), F32),
            pltpu.VMEM((7, 4, 8, BLK), F32),
            pltpu.SemaphoreType.DMA((14,)),
            pltpu.SemaphoreType.DMA((4, 26)),
            pltpu.SemaphoreType.DMA((4, 26)),
            pltpu.SemaphoreType.DMA((4, 4)),
            pltpu.SemaphoreType.DMA((4, 4)),
            pltpu.SemaphoreType.DMA((4, 8)),
            pltpu.SemaphoreType.DMA((4, 8)),
            pltpu.SemaphoreType.DMA((13,)),
            pltpu.SemaphoreType.DMA((13,)),
        ],
        compiler_params=pltpu.CompilerParams(
            collective_id=0, has_side_effects=True, vmem_limit_bytes=60 * 1024 * 1024
        ),
        name="outer_step",
    )(
        lines(positions, 3),
        lines(velocities, 3),
        strength.reshape(NB, 1, BLK),
        charge.reshape(NB, 1, BLK),
        lines(bond_stiffness, 2),
        lines(bond_partner, 2),
        lines(bond_force, 3),
        lines(pair_force, 3),
        lines(far_force, 3),
        cell_frac,
        pair_blocks.reshape(NB, 8).T,
        block_cell.reshape(NB),
        tile_count.reshape(1),
    )
    return xv[:3].reshape(positions.shape), xv[3:].reshape(velocities.shape)


def solution(mesh):
    vector = P(None, "gx", "gy", "gz", None)
    scalar = P("gx", "gy", "gz", None)
    in_specs = (
        vector,
        vector,
        scalar,
        scalar,
        vector,
        vector,
        P("gx", "gy", "gz", None, None),
        P("gx", "gy", "gz"),
        scalar,
        P(),
        vector,
        vector,
        vector,
    )
    return jax.shard_map(
        per_device, mesh=mesh, in_specs=in_specs, out_specs=(vector, vector), check_vma=False
    )
```

```python
import math

import jax
import jax.numpy as jnp
from jax import lax
from jax.experimental import pallas as pl
from jax.experimental.pallas import tpu as pltpu
from jax.sharding import PartitionSpec as P

MESH = pl.DeviceIdType.MESH
SBX, SBY, SBZ = 4, 4, 2
BLK = 128
NB = SBX * SBY * SBZ
EX, EY, EZ = SBX + 2, SBY + 2, SBZ + 2
NE = EX * EY * EZ
CELLS = 1024
AXES = ("gx", "gy", "gz")

inner_step = 0.1
gauss_width = 0.25
pair_scale = 0.1
soften = 1.0
coulomb = 0.02
half_step = 0.5 * inner_step
outer_half = 2.0 * inner_step

rate = 1.0 / (2.0 * gauss_width * gauss_width)
bits = rate / math.log(2.0)
pair_factor = pair_scale / (gauss_width * gauss_width) * math.exp(-rate) / (bits * bits)

FACES = ((-1, 0, 0), (1, 0, 0), (0, -1, 0), (0, 1, 0), (0, 0, -1), (0, 0, 1))
AROUND = tuple(
    (dx, dy, dz)
    for dx in (-1, 0, 1)
    for dy in (-1, 0, 1)
    for dz in (-1, 0, 1)
    if (dx, dy, dz) != (0, 0, 0)
)
SIZES = (4, 8, 4)

F32 = jnp.float32
BF16 = jnp.bfloat16


def row_ids(n=4):
    return lax.broadcasted_iota(jnp.int32, (n, BLK), 0)


def rows4(a, b, c, d):
    r = row_ids()
    return jnp.where(r == 0, a, jnp.where(r == 1, b, jnp.where(r == 2, c, d)))


def place(b):
    return b // (SBY * SBZ) + 1, b // SBZ % SBY + 1, b % SBZ + 1


def lane_gather(values, lanes):
    numbers = lax.GatherDimensionNumbers(
        offset_dims=(),
        collapsed_slice_dims=(1,),
        start_index_map=(1,),
        operand_batching_dims=(0,),
        start_indices_batching_dims=(0,),
    )
    return lax.gather(
        values,
        lanes[..., None],
        numbers,
        slice_sizes=(1, 1),
        mode=lax.GatherScatterMode.PROMISE_IN_BOUNDS,
    )


def thirds(value):
    high = value.astype(BF16).astype(F32)
    rest = value - high
    middle = rest.astype(BF16).astype(F32)
    return high, middle, rest - middle


def send_box(step, inner, ghost):
    count = inner
    if step == 0:
        return 1, count
    if ghost:
        return (0 if step > 0 else count + 1), 1
    return (count if step > 0 else 1), 1


def box(direction, ghost):
    return [send_box(s, inner, ghost) for s, inner in zip(direction, (SBX, SBY, SBZ))]


def part_box(direction, ghost, rows):
    where = box(direction, ghost)
    if direction[1] == 0:
        where[1] = (rows[0] + 1, rows[1])
    return where


def cut(where, lines=4):
    return tuple(pl.ds(start, size) for start, size in where) + (pl.ds(0, lines), slice(None))


def spots(where):
    (x, nx), (y, ny), (z, nz) = where
    return [(x + i, y + j, z + k) for i in range(nx) for j in range(ny) for k in range(nz)]


def flat(x, y, z):
    return (x * EY + y) * EZ + z


ORDER = sorted(AROUND, key=lambda d: (d[1] != 0, d[2] != 0, d))
SENDS = ORDER[::-1]
ORDER_Y = next(i for i, d in enumerate(ORDER) if d[1] != 0)


def kernel(
    pos_h,
    vel_h,
    stren_h,
    chg_h,
    stiff_h,
    part_h,
    bforce_h,
    pforce_h,
    fforce_h,
    frac_h,
    pairs_h,
    cell_h,
    count_h,
    oo,
    pos,
    vel,
    stren,
    chg,
    stiff,
    part,
    bforce,
    pforce,
    fforce,
    frac,
    frac_s,
    pairs,
    cell,
    count,
    hood0,
    hood1,
    hood2,
    hood3,
    vbuf,
    qbuf,
    slots,
    aways,
    springs,
    near,
    pull,
    left,
    centre,
    part0,
    part1,
    part2,
    got0,
    got1,
    got2,
    ins,
    hs,
    hr,
    gs,
    gr,
    rs,
    rr,
    ms,
    mr,
):
    me = tuple(lax.axis_index(a) for a in AXES)

    def device(shift):
        return tuple(lax.rem(m + (s + n), n) for m, s, n in zip(me, shift, SIZES))

    barrier = pltpu.get_barrier_semaphore()
    peers = set(AROUND)
    for axis, n in ((2, 4), (0, 4), (1, 8)):
        for o in range(2, n - 1):
            peers.add(tuple(o if a == axis else 0 for a in range(3)))
    peers = sorted(peers)
    for shift in peers:
        pl.semaphore_signal(barrier, inc=1, device_id=device(shift), device_id_type=MESH)

    fetches = [
        pltpu.make_async_copy(source, target, ins.at[i])
        for i, (source, target) in enumerate(
            (
                (count_h, count),
                (pos_h, pos),
                (vel_h, vel),
                (fforce_h, fforce),
                (pforce_h, pforce),
                (bforce_h, bforce),
                (stren_h, stren),
                (part_h, part),
                (stiff_h, stiff),
                (chg_h, chg),
                (pairs_h, pairs),
                (cell_h, cell),
                (frac_h, frac),
                (frac_h, frac_s),
            )
        )
    ]
    for copy in fetches:
        copy.start()

    rows = row_ids()
    xyz = rows < 3
    lanes = lax.broadcasted_iota(jnp.int32, (1, BLK), 1)
    rows8 = row_ids(8)
    upper = rows8 < 4

    def halo(hood, which, directions, lines):
        return {
            d: pltpu.make_async_remote_copy(
                src_ref=hood.at[cut(box(d, False), lines)],
                dst_ref=hood.at[cut(box(d, True), lines)],
                send_sem=hs.at[which, AROUND.index(d)],
                recv_sem=hr.at[which, AROUND.index(d)],
                device_id=device(d),
                device_id_type=MESH,
            )
            for d in directions
        }

    def launch(copies):
        for d in SENDS:
            if d in copies:
                copies[d].start()

    def shift_of(d):
        return rows4(-SBX * d[0] * 1.0, -SBY * d[1] * 1.0, -SBZ * d[2] * 1.0, 0.0)

    def begin(b, _):
        px, py, pz = place(b)
        live = jnp.where(b * BLK + lanes < count[0], 1.0, 0.0)
        x = rows4(pos[0, b], pos[1, b], pos[2, b], stren[b] * live)
        v = [
            vel[d, b]
            + outer_half * fforce[d, b]
            + inner_step * pforce[d, b]
            + half_step * bforce[d, b]
            for d in range(3)
        ]
        v = rows4(v[0], v[1], v[2], 0.0)
        vbuf[b] = v
        hood0[px, py, pz] = x + inner_step * v
        return 0

    for copy in fetches[:7]:
        copy.wait()
    lax.fori_loop(0, NB, begin, 0, unroll=4)
    pl.semaphore_wait(barrier, len(peers))
    copies0 = halo(hood0, 0, FACES, 3)
    launch(copies0)

    for copy in fetches[7:]:
        copy.wait()

    def bonds(b, _):
        px, py, pz = place(b)
        live = jnp.where(b * BLK + lanes < count[0], 1.0, 0.0)
        qbuf[b] = chg[b] * live
        columns = jnp.where(upper, part[0, b], part[1, b])
        slots[b] = columns & (BLK - 1)
        aways[b] = jnp.where((rows8 & 3) < 3, (columns >> 7) - flat(px, py, pz), NE)
        spring = jnp.where(upper, stiff[0, b], stiff[1, b])
        springs[b] = jnp.where((rows8 & 3) < 3, spring, 0.0)
        return 0

    lax.fori_loop(0, NB, bonds, 0, unroll=4)
    for d in range(3):
        for k in range(8):
            centre[d, k : k + 1, :] = frac[d : d + 1, k * BLK : (k + 1) * BLK] * (
                1.0 * SIZES[d] * (SBX, SBY, SBZ)[d]
            )

    def pick(tile, b, d):
        twice = jnp.concatenate([tile, tile], axis=0)
        offset = (d[0] * EY + d[1]) * EZ + d[2]
        return twice, aways[b] == offset, lane_gather(twice, slots[b])

    def fold(value):
        return value[0:4] + value[4:8]

    def bond_inside(hood, size):
        for b in range(NB):
            p = tuple(int(i) for i in place(b))
            own, hit, other = pick(hood[p], b, (0, 0, 0))
            other = jnp.where(hit, other, 0.0)
            for d in FACES:
                q = tuple(i + j for i, j in zip(p, d))
                if all(1 <= i <= n for i, n in zip(q, (SBX, SBY, SBZ))):
                    _, hit, value = pick(hood[q], b, d)
                    other = jnp.where(hit, value, other)
            vbuf[b] = vbuf[b] + size * fold(springs[b] * (other - own))

    def bond_face(hood, size, d, rows=(0, SBY)):
        shift = shift_of(d)
        for q in spots(part_box(d, True, rows)):
            e = tuple(-i for i in d)
            p = tuple(i + j for i, j in zip(q, d))
            b = ((p[0] - 1) * SBY + p[1] - 1) * SBZ + p[2] - 1
            _, hit, value = pick(hood[q] + shift, b, e)
            vbuf[b] = vbuf[b] + size * fold(jnp.where(hit, springs[b] * value, 0.0))

    def drift(hood, after, row=None):
        for b in range(NB):
            p = tuple(int(i) for i in place(b))
            if row is None or p[1] == row + 1:
                after[p] = hood[p] + inner_step * vbuf[b]

    middle = rows4(0.5 * SBX, 0.5 * SBY, 0.5 * SBZ, 0.0)
    ones = jnp.where(xyz, 1.0, 0.0)
    blank = jnp.zeros((4, BLK), F32)

    def square_sum(z):
        return jnp.sum(jnp.where(xyz, z * z, 0.0), axis=0, keepdims=True)

    def prepare(e, z, a):
        high, mid, low = thirds(jnp.where(xyz, z, -bits * square_sum(z)))
        near[e] = jnp.concatenate(
            [high, mid, low, high, mid, high, ones, blank], axis=0
        ).astype(BF16)
        high, mid, low = thirds(jnp.where(xyz, z * a, a))
        pull[e] = jnp.concatenate([high, mid, low, blank], axis=0).astype(BF16)

    def prepare_ghosts(hood, d, rows=(0, SBY)):
        shift = shift_of(d) - middle
        for q in spots(part_box(d, True, rows)):
            prepare(flat(*q), hood[q] + shift, hood1[q][3:4])

    def prepare_own(hood):
        def body(b, _):
            px, py, pz = place(b)
            tile = hood[px, py, pz]
            z = tile - middle
            prepare(flat(px, py, pz), z, tile[3:4])
            high, mid, low = thirds(jnp.where(xyz, (2.0 * bits) * z, 1.0))
            ph, pm, pw = thirds(bits - bits * square_sum(z))
            stack = jnp.concatenate(
                [high, high, high, mid, mid, low, rows4(ph, pm, pw, 0.0), blank], axis=0
            )
            left[b] = stack.T.astype(BF16)
            return 0

        lax.fori_loop(0, NB, body, 0, unroll=8)

    def pair(hood, c, p):
        listed = [pairs[k, c] for k in range(8)]
        t = jnp.dot(
            left[c],
            jnp.concatenate([near[e] for e in listed], axis=1),
            preferred_element_type=F32,
        )
        r = jnp.maximum(t, 0.0)
        w = jnp.exp2(t) * (r * r)
        high = w.astype(BF16)
        low = (w - high.astype(F32)).astype(BF16)
        y = jnp.concatenate([pull[e] for e in listed], axis=1)
        over = (((1,), (1,)), ((), ()))
        both = lax.dot_general(
            jnp.concatenate([high, low], axis=0), y, over, preferred_element_type=F32
        )
        acc = both[0:BLK] + both[BLK : 2 * BLK]
        s = acc.T
        f = s[0:4] + s[4:8] + s[8:12]
        tile = hood[p]
        z = tile - middle
        force = (pair_factor * tile[3:4]) * (z * f[3:4] - f)
        return tile, jnp.where(xyz, force, 0.0)

    def pair_row(hood, by, body):
        for bx in range(SBX):
            for bz in range(SBZ):
                c = (bx * SBY + by) * SBZ + bz
                p = (bx + 1, by + 1, bz + 1)
                body(c, p, *pair(hood, c, p))

    bond_inside(hood0, inner_step)
    for d in ORDER:
        if d in copies0:
            copies0[d].wait_recv()
            bond_face(hood0, inner_step, d)
    drift(hood0, hood1)
    copies1 = halo(hood1, 1, AROUND, 4)
    launch(copies1)
    prepare_own(hood1)
    bond_inside(hood1, inner_step)
    def take1(d):
        copies1[d].wait_recv()
        prepare_ghosts(hood1, d)
        if d in FACES:
            bond_face(hood1, inner_step, d)

    def row_copies(hood, directions, by, sends, recvs):
        rows = (by, 1)
        return {
            d: pltpu.make_async_remote_copy(
                src_ref=hood.at[cut(part_box(d, False, rows), 3)],
                dst_ref=hood.at[cut(part_box(d, True, rows), 3)],
                send_sem=sends.at[by, i],
                recv_sem=recvs.at[by, i],
                device_id=device(d),
                device_id_type=MESH,
            )
            for i, d in enumerate(directions)
        }

    flat_faces = [d for d in FACES if d[1] == 0]
    copies2 = halo(hood2, 2, ((0, -1, 0), (0, 1, 0)), 3)
    parts2 = [row_copies(hood2, flat_faces, by, gs, gr) for by in range(SBY)]

    def kick_drift(c, p, tile, force):
        v = vbuf[c] + (2.0 * inner_step) * force
        vbuf[c] = v
        hood2[p] = tile + inner_step * v

    for d in ORDER[:ORDER_Y]:
        take1(d)

    def first_row(g, _):
        by = jnp.where(g == 0, 1, jnp.where(g == 1, 0, jnp.where(g == 2, SBY - 1, 2)))
        pair_row(hood1, by, kick_drift)

        @pl.when(g == 0)
        def _():
            for d in ORDER[ORDER_Y:]:
                take1(d)

        @pl.when(g == 1)
        def _():
            copies2[(0, -1, 0)].start()

        @pl.when(g == 2)
        def _():
            copies2[(0, 1, 0)].start()

        for copy in row_copies(hood2, flat_faces, by, gs, gr).values():
            copy.start()
        return 0

    lax.fori_loop(0, SBY, first_row, 0)
    copies3 = halo(hood3, 3, [d for d in AROUND if d[1] != 0], 3)
    flat_around = [d for d in AROUND if d[1] == 0]
    parts3 = [row_copies(hood3, flat_around, by, rs, rr) for by in range(SBY)]
    bond_inside(hood2, inner_step)
    for by in (1, SBY - 1, 0, 2):
        for d in flat_faces:
            parts2[by][d].wait_recv()
            bond_face(hood2, inner_step, d, (by, 1))
        if by in (0, SBY - 1):
            d = (0, 1, 0) if by == 0 else (0, -1, 0)
            copies2[d].wait_recv()
            bond_face(hood2, inner_step, d)
        drift(hood2, hood3, by)
        if by in (0, SBY - 1):
            launch({d: copies3[d] for d in copies3 if d[1] == (-1 if by == 0 else 1)})
        launch(parts3[by])
    cell_ids = lax.broadcasted_iota(jnp.int32, (8, BLK), 0) * BLK + lax.broadcasted_iota(
        jnp.int32, (8, BLK), 1
    )
    corner = rows4(
        (me[0] * SBX).astype(F32), (me[1] * SBY).astype(F32), (me[2] * SBZ).astype(F32), 0.0
    )

    def gather_moments(b, totals):
        px, py, pz = place(b)
        tile = hood3[px, py, pz]
        for d in range(3):
            oo[d, b] = tile[d : d + 1]
        sums = jnp.sum(
            qbuf[b] * jnp.where(xyz, tile + corner, 1.0), axis=1, keepdims=True
        )
        here = cell_ids == cell[b]
        return tuple(
            total + jnp.where(here, sums[d : d + 1], 0.0) for d, total in enumerate(totals)
        )

    zero = jnp.zeros((8, BLK), F32)
    moments = lax.fori_loop(0, NB, gather_moments, (zero, zero, zero, zero), unroll=16)
    for d in range(4):
        part0[d] = moments[d]

    stages = ((2, 4, part0, got0, 0), (0, 4, part1, got1, 3), (1, 8, part2, got2, 6))

    def spread(stage):
        axis, n, mine, got, base = stages[stage]
        return [
            pltpu.make_async_remote_copy(
                src_ref=mine,
                dst_ref=got.at[o - 1],
                send_sem=ms.at[base + o - 1],
                recv_sem=mr.at[base + o - 1],
                device_id=device(tuple(o if a == axis else 0 for a in range(3))),
                device_id_type=MESH,
            )
            for o in range(1, n)
        ]

    spreads = [spread(stage) for stage in range(3)]

    def send_moments(stage):
        for copy in spreads[stage]:
            copy.start()

    def collect(stage):
        axis, n, mine, got, base = stages[stage]
        for copy in spreads[stage]:
            copy.wait_recv()
        total = mine[...]
        for o in range(1, n):
            total = total + got[o - 1]
        return total

    send_moments(0)
    prepare_own(hood3)
    bond_inside(hood3, half_step)

    def take3(copies, d, rows=(0, SBY)):
        copies[d].wait_recv()
        prepare_ghosts(hood3, d, rows)
        if d in FACES:
            bond_face(hood3, half_step, d, rows)

    def kick(c, p, tile, force):
        vbuf[c] = vbuf[c] + inner_step * force

    for by in (1, SBY - 1, 0):
        for d in flat_around:
            take3(parts3[by], d, (by, 1))
    for d in ORDER[ORDER_Y:]:
        if d[1] > 0:
            take3(copies3, d)

    def second_row(by, _):
        pair_row(hood3, by, kick)

        @pl.when(by == 0)
        def _():
            part1[...] = collect(0)
            send_moments(1)
            for d in flat_around:
                take3(parts3[2], d, (2, 1))
            for d in ORDER[ORDER_Y:]:
                if d[1] < 0:
                    take3(copies3, d)

        @pl.when(by == 1)
        def _():
            part2[...] = collect(1)
            send_moments(2)

        return 0

    lax.fori_loop(0, SBY, second_row, 0)
    totals = collect(2)

    charge_sum = totals[3]
    places = [centre[d] for d in range(3)]
    dipole = [totals[d] - charge_sum * places[d] for d in range(3)]

    def finish(b, _):
        target = cell[b]
        away = [
            frac_s[d, target] * (1.0 * SIZES[d] * (SBX, SBY, SBZ)[d]) - places[d]
            for d in range(3)
        ]
        inverse = lax.rsqrt(
            away[0] * away[0] + away[1] * away[1] + away[2] * away[2] + soften * soften
        )
        cube = inverse * inverse * inverse
        fifth = cube * inverse * inverse
        along = dipole[0] * away[0] + dipole[1] * away[1] + dipole[2] * away[2]
        gain = charge_sum * cube + 3.0 * along * fifth
        field = [
            jnp.sum(gain * away[d] - dipole[d] * cube, axis=(0, 1), keepdims=True)
            for d in range(3)
        ]
        size = (outer_half * coulomb) * qbuf[b]
        v = vbuf[b]
        for d in range(3):
            oo[3 + d, b] = v[d : d + 1] + size * field[d]
        return 0

    lax.fori_loop(0, NB, finish, 0, unroll=32)

    sent = [copies[d] for copies in (copies0, copies1, copies2, copies3) for d in copies]
    for copies in parts2 + parts3:
        sent += copies.values()
    for copies in spreads:
        sent += copies
    for copy in sent:
        copy.wait_send()


def per_device(
    positions,
    velocities,
    strength,
    charge,
    bond_stiffness,
    bond_partner,
    pair_blocks,
    tile_count,
    block_cell,
    cell_frac,
    bond_force,
    pair_force,
    far_force,
):
    lines = lambda value, n: value.reshape(n, NB, 1, BLK)
    vmem = pl.BlockSpec(memory_space=pltpu.VMEM)
    anywhere = pl.BlockSpec(memory_space=pl.ANY)
    hood = pltpu.VMEM((EX, EY, EZ, 4, BLK), F32)
    line3 = pltpu.VMEM((3, NB, 1, BLK), F32)
    line2 = pltpu.VMEM((2, NB, 1, BLK), F32)
    line1 = pltpu.VMEM((NB, 1, BLK), F32)
    sums = pltpu.VMEM((4, 8, BLK), F32)
    out = jax.ShapeDtypeStruct((3, NB, 1, BLK), F32)
    xv = pl.pallas_call(
        kernel,
        out_shape=jax.ShapeDtypeStruct((6, NB, 1, BLK), F32),
        in_specs=[anywhere] * 13,
        out_specs=vmem,
        scratch_shapes=[
            line3,
            line3,
            line1,
            line1,
            line2,
            pltpu.VMEM((2, NB, 1, BLK), jnp.int32),
            line3,
            line3,
            line3,
            pltpu.VMEM((3, CELLS), F32),
            pltpu.SMEM((3, CELLS), F32),
            pltpu.SMEM((8, NB), jnp.int32),
            pltpu.SMEM((NB,), jnp.int32),
            pltpu.SMEM((1,), jnp.int32),
            hood,
            hood,
            hood,
            hood,
            pltpu.VMEM((NB, 4, BLK), F32),
            line1,
            pltpu.VMEM((NB, 8, BLK), jnp.int32),
            pltpu.VMEM((NB, 8, BLK), jnp.int32),
            pltpu.VMEM((NB, 8, BLK), F32),
            pltpu.VMEM((NE, 32, BLK), BF16),
            pltpu.VMEM((NE, 16, BLK), BF16),
            pltpu.VMEM((NB, BLK, 32), BF16),
            pltpu.VMEM((3, 8, BLK), F32),
            sums,
            sums,
            sums,
            pltpu.VMEM((3, 4, 8, BLK), F32),
            pltpu.VMEM((3, 4, 8, BLK), F32),
            pltpu.VMEM((7, 4, 8, BLK), F32),
            pltpu.SemaphoreType.DMA((14,)),
            pltpu.SemaphoreType.DMA((4, 26)),
            pltpu.SemaphoreType.DMA((4, 26)),
            pltpu.SemaphoreType.DMA((4, 4)),
            pltpu.SemaphoreType.DMA((4, 4)),
            pltpu.SemaphoreType.DMA((4, 8)),
            pltpu.SemaphoreType.DMA((4, 8)),
            pltpu.SemaphoreType.DMA((13,)),
            pltpu.SemaphoreType.DMA((13,)),
        ],
        compiler_params=pltpu.CompilerParams(
            collective_id=0, has_side_effects=True, vmem_limit_bytes=60 * 1024 * 1024
        ),
        name="outer_step",
    )(
        lines(positions, 3),
        lines(velocities, 3),
        strength.reshape(NB, 1, BLK),
        charge.reshape(NB, 1, BLK),
        lines(bond_stiffness, 2),
        lines(bond_partner, 2),
        lines(bond_force, 3),
        lines(pair_force, 3),
        lines(far_force, 3),
        cell_frac,
        pair_blocks.reshape(NB, 8).T,
        block_cell.reshape(NB),
        tile_count.reshape(1),
    )
    return xv[:3].reshape(positions.shape), xv[3:].reshape(velocities.shape)


def solution(mesh):
    vector = P(None, "gx", "gy", "gz", None)
    scalar = P("gx", "gy", "gz", None)
    in_specs = (
        vector,
        vector,
        scalar,
        scalar,
        vector,
        vector,
        P("gx", "gy", "gz", None, None),
        P("gx", "gy", "gz"),
        scalar,
        P(),
        vector,
        vector,
        vector,
    )
    return jax.shard_map(
        per_device, mesh=mesh, in_specs=in_specs, out_specs=(vector, vector), check_vma=False
    )
```

```python
import math

import jax
import jax.numpy as jnp
from jax import lax
from jax.experimental import pallas as pl
from jax.experimental.pallas import tpu as pltpu
from jax.sharding import PartitionSpec as P

MESH = pl.DeviceIdType.MESH
SBX, SBY, SBZ = 4, 4, 2
BLK = 128
NB = SBX * SBY * SBZ
EX, EY, EZ = SBX + 2, SBY + 2, SBZ + 2
NE = EX * EY * EZ
CELLS = 1024
AXES = ("gx", "gy", "gz")

inner_step = 0.1
gauss_width = 0.25
pair_scale = 0.1
soften = 1.0
coulomb = 0.02
half_step = 0.5 * inner_step
outer_half = 2.0 * inner_step

rate = 1.0 / (2.0 * gauss_width * gauss_width)
bits = rate / math.log(2.0)
pair_factor = pair_scale / (gauss_width * gauss_width) * math.exp(-rate) / (bits * bits)

FACES = ((-1, 0, 0), (1, 0, 0), (0, -1, 0), (0, 1, 0), (0, 0, -1), (0, 0, 1))
AROUND = tuple(
    (dx, dy, dz)
    for dx in (-1, 0, 1)
    for dy in (-1, 0, 1)
    for dz in (-1, 0, 1)
    if (dx, dy, dz) != (0, 0, 0)
)
SIZES = (4, 8, 4)

F32 = jnp.float32
BF16 = jnp.bfloat16


def row_ids(n=4):
    return lax.broadcasted_iota(jnp.int32, (n, BLK), 0)


def rows4(a, b, c, d):
    r = row_ids()
    return jnp.where(r == 0, a, jnp.where(r == 1, b, jnp.where(r == 2, c, d)))


def place(b):
    return b // (SBY * SBZ) + 1, b // SBZ % SBY + 1, b % SBZ + 1


def lane_gather(values, lanes):
    numbers = lax.GatherDimensionNumbers(
        offset_dims=(),
        collapsed_slice_dims=(1,),
        start_index_map=(1,),
        operand_batching_dims=(0,),
        start_indices_batching_dims=(0,),
    )
    return lax.gather(
        values,
        lanes[..., None],
        numbers,
        slice_sizes=(1, 1),
        mode=lax.GatherScatterMode.PROMISE_IN_BOUNDS,
    )


def thirds(value):
    high = value.astype(BF16).astype(F32)
    rest = value - high
    middle = rest.astype(BF16).astype(F32)
    return high, middle, rest - middle


def send_box(step, inner, ghost):
    count = inner
    if step == 0:
        return 1, count
    if ghost:
        return (0 if step > 0 else count + 1), 1
    return (count if step > 0 else 1), 1


def box(direction, ghost):
    return [send_box(s, inner, ghost) for s, inner in zip(direction, (SBX, SBY, SBZ))]


def part_box(direction, ghost, rows):
    where = box(direction, ghost)
    if direction[1] == 0:
        where[1] = (rows[0] + 1, rows[1])
    return where


def cut(where, lines=4):
    return tuple(pl.ds(start, size) for start, size in where) + (pl.ds(0, lines), slice(None))


def spots(where):
    (x, nx), (y, ny), (z, nz) = where
    return [(x + i, y + j, z + k) for i in range(nx) for j in range(ny) for k in range(nz)]


def flat(x, y, z):
    return (x * EY + y) * EZ + z


ORDER = sorted(AROUND, key=lambda d: (d[1] != 0, d[2] != 0, d))
SENDS = ORDER[::-1]
ORDER_Y = next(i for i, d in enumerate(ORDER) if d[1] != 0)


def kernel(
    pos_h,
    vel_h,
    stren_h,
    chg_h,
    stiff_h,
    part_h,
    bforce_h,
    pforce_h,
    fforce_h,
    frac_h,
    pairs_h,
    cell_h,
    count_h,
    oo,
    pos,
    vel,
    stren,
    chg,
    stiff,
    part,
    bforce,
    pforce,
    fforce,
    frac,
    frac_s,
    pairs,
    cell,
    count,
    hood0,
    hood1,
    hood2,
    hood3,
    vbuf,
    qbuf,
    slots,
    aways,
    springs,
    near,
    pull,
    left,
    centre,
    part0,
    part1,
    part2,
    got0,
    got1,
    got2,
    ins,
    hs,
    hr,
    gs,
    gr,
    rs,
    rr,
    ms,
    mr,
):
    me = tuple(lax.axis_index(a) for a in AXES)

    def device(shift):
        return tuple(lax.rem(m + (s + n), n) for m, s, n in zip(me, shift, SIZES))

    barrier = pltpu.get_barrier_semaphore()
    peers = set(AROUND)
    for axis, n in ((2, 4), (0, 4), (1, 8)):
        for o in range(2, n - 1):
            peers.add(tuple(o if a == axis else 0 for a in range(3)))
    peers = sorted(peers)
    for shift in peers:
        pl.semaphore_signal(barrier, inc=1, device_id=device(shift), device_id_type=MESH)

    fetches = [
        pltpu.make_async_copy(source, target, ins.at[i])
        for i, (source, target) in enumerate(
            (
                (count_h, count),
                (pos_h, pos),
                (vel_h, vel),
                (fforce_h, fforce),
                (pforce_h, pforce),
                (bforce_h, bforce),
                (stren_h, stren),
                (part_h, part),
                (stiff_h, stiff),
                (chg_h, chg),
                (pairs_h, pairs),
                (cell_h, cell),
                (frac_h, frac),
                (frac_h, frac_s),
            )
        )
    ]
    for copy in fetches:
        copy.start()

    rows = row_ids()
    xyz = rows < 3
    lanes = lax.broadcasted_iota(jnp.int32, (1, BLK), 1)
    rows8 = row_ids(8)
    upper = rows8 < 4

    def halo(hood, which, directions, lines):
        return {
            d: pltpu.make_async_remote_copy(
                src_ref=hood.at[cut(box(d, False), lines)],
                dst_ref=hood.at[cut(box(d, True), lines)],
                send_sem=hs.at[which, AROUND.index(d)],
                recv_sem=hr.at[which, AROUND.index(d)],
                device_id=device(d),
                device_id_type=MESH,
            )
            for d in directions
        }

    def launch(copies):
        for d in SENDS:
            if d in copies:
                copies[d].start()

    def drained(groups):
        for group in groups:
            for copy in group.values() if isinstance(group, dict) else group:
                copy.wait_send()

    def shift_of(d):
        return rows4(-SBX * d[0] * 1.0, -SBY * d[1] * 1.0, -SBZ * d[2] * 1.0, 0.0)

    def begin(b, _):
        px, py, pz = place(b)
        live = jnp.where(b * BLK + lanes < count[0], 1.0, 0.0)
        x = rows4(pos[0, b], pos[1, b], pos[2, b], stren[b] * live)
        v = [
            vel[d, b]
            + outer_half * fforce[d, b]
            + inner_step * pforce[d, b]
            + half_step * bforce[d, b]
            for d in range(3)
        ]
        v = rows4(v[0], v[1], v[2], 0.0)
        vbuf[b] = v
        hood0[px, py, pz] = x + inner_step * v
        return 0

    for copy in fetches[:7]:
        copy.wait()
    lax.fori_loop(0, NB, begin, 0, unroll=4)
    pl.semaphore_wait(barrier, len(peers))
    copies0 = halo(hood0, 0, FACES, 3)
    launch(copies0)

    for copy in fetches[7:]:
        copy.wait()

    def bonds(b, _):
        px, py, pz = place(b)
        live = jnp.where(b * BLK + lanes < count[0], 1.0, 0.0)
        qbuf[b] = chg[b] * live
        columns = jnp.where(upper, part[0, b], part[1, b])
        slots[b] = columns & (BLK - 1)
        aways[b] = jnp.where((rows8 & 3) < 3, (columns >> 7) - flat(px, py, pz), NE)
        spring = jnp.where(upper, stiff[0, b], stiff[1, b])
        springs[b] = jnp.where((rows8 & 3) < 3, spring, 0.0)
        return 0

    lax.fori_loop(0, NB, bonds, 0, unroll=4)
    for d in range(3):
        for k in range(8):
            centre[d, k : k + 1, :] = frac[d : d + 1, k * BLK : (k + 1) * BLK] * (
                1.0 * SIZES[d] * (SBX, SBY, SBZ)[d]
            )

    def pick(tile, b, d):
        twice = jnp.concatenate([tile, tile], axis=0)
        offset = (d[0] * EY + d[1]) * EZ + d[2]
        return twice, aways[b] == offset, lane_gather(twice, slots[b])

    def fold(value):
        return value[0:4] + value[4:8]

    def bond_inside(hood, size):
        for b in range(NB):
            p = tuple(int(i) for i in place(b))
            own, hit, other = pick(hood[p], b, (0, 0, 0))
            other = jnp.where(hit, other, 0.0)
            for d in FACES:
                q = tuple(i + j for i, j in zip(p, d))
                if all(1 <= i <= n for i, n in zip(q, (SBX, SBY, SBZ))):
                    _, hit, value = pick(hood[q], b, d)
                    other = jnp.where(hit, value, other)
            vbuf[b] = vbuf[b] + size * fold(springs[b] * (other - own))

    def bond_face(hood, size, d, rows=(0, SBY)):
        shift = shift_of(d)
        for q in spots(part_box(d, True, rows)):
            e = tuple(-i for i in d)
            p = tuple(i + j for i, j in zip(q, d))
            b = ((p[0] - 1) * SBY + p[1] - 1) * SBZ + p[2] - 1
            _, hit, value = pick(hood[q] + shift, b, e)
            vbuf[b] = vbuf[b] + size * fold(jnp.where(hit, springs[b] * value, 0.0))

    def drift(hood, after, row=None):
        for b in range(NB):
            p = tuple(int(i) for i in place(b))
            if row is None or p[1] == row + 1:
                after[p] = hood[p] + inner_step * vbuf[b]

    middle = rows4(0.5 * SBX, 0.5 * SBY, 0.5 * SBZ, 0.0)
    ones = jnp.where(xyz, 1.0, 0.0)
    blank = jnp.zeros((4, BLK), F32)

    def square_sum(z):
        return jnp.sum(jnp.where(xyz, z * z, 0.0), axis=0, keepdims=True)

    def prepare(e, z, a):
        high, mid, low = thirds(jnp.where(xyz, z, -bits * square_sum(z)))
        near[e] = jnp.concatenate(
            [high, mid, low, high, mid, high, ones, blank], axis=0
        ).astype(BF16)
        high, mid, low = thirds(jnp.where(xyz, z * a, a))
        pull[e] = jnp.concatenate([high, mid, low, blank], axis=0).astype(BF16)

    def prepare_ghosts(hood, d, rows=(0, SBY)):
        shift = shift_of(d) - middle
        for q in spots(part_box(d, True, rows)):
            prepare(flat(*q), hood[q] + shift, hood1[q][3:4])

    def prepare_own(hood):
        def body(b, _):
            px, py, pz = place(b)
            tile = hood[px, py, pz]
            z = tile - middle
            prepare(flat(px, py, pz), z, tile[3:4])
            high, mid, low = thirds(jnp.where(xyz, (2.0 * bits) * z, 1.0))
            ph, pm, pw = thirds(bits - bits * square_sum(z))
            stack = jnp.concatenate(
                [high, high, high, mid, mid, low, rows4(ph, pm, pw, 0.0), blank], axis=0
            )
            left[b] = stack.T.astype(BF16)
            return 0

        lax.fori_loop(0, NB, body, 0, unroll=8)

    def pair(hood, c, p):
        listed = [pairs[k, c] for k in range(8)]
        t = jnp.dot(
            left[c],
            jnp.concatenate([near[e] for e in listed], axis=1),
            preferred_element_type=F32,
        )
        r = jnp.maximum(t, 0.0)
        w = jnp.exp2(t) * (r * r)
        high = w.astype(BF16)
        low = (w - high.astype(F32)).astype(BF16)
        y = jnp.concatenate([pull[e] for e in listed], axis=1)
        over = (((1,), (1,)), ((), ()))
        both = lax.dot_general(
            jnp.concatenate([high, low], axis=0), y, over, preferred_element_type=F32
        )
        acc = both[0:BLK] + both[BLK : 2 * BLK]
        s = acc.T
        f = s[0:4] + s[4:8] + s[8:12]
        tile = hood[p]
        z = tile - middle
        force = (pair_factor * tile[3:4]) * (z * f[3:4] - f)
        return tile, jnp.where(xyz, force, 0.0)

    def pair_row(hood, by, body):
        for bx in range(SBX):
            for bz in range(SBZ):
                c = (bx * SBY + by) * SBZ + bz
                p = (bx + 1, by + 1, bz + 1)
                body(c, p, *pair(hood, c, p))

    bond_inside(hood0, inner_step)
    for d in ORDER:
        if d in copies0:
            copies0[d].wait_recv()
            bond_face(hood0, inner_step, d)
    drift(hood0, hood1)
    copies1 = halo(hood1, 1, AROUND, 4)
    launch(copies1)
    drained([copies0])
    prepare_own(hood1)
    bond_inside(hood1, inner_step)
    def take1(d):
        copies1[d].wait_recv()
        prepare_ghosts(hood1, d)
        if d in FACES:
            bond_face(hood1, inner_step, d)

    def row_copies(hood, directions, by, sends, recvs):
        rows = (by, 1)
        return {
            d: pltpu.make_async_remote_copy(
                src_ref=hood.at[cut(part_box(d, False, rows), 3)],
                dst_ref=hood.at[cut(part_box(d, True, rows), 3)],
                send_sem=sends.at[by, i],
                recv_sem=recvs.at[by, i],
                device_id=device(d),
                device_id_type=MESH,
            )
            for i, d in enumerate(directions)
        }

    flat_faces = [d for d in FACES if d[1] == 0]
    copies2 = halo(hood2, 2, ((0, -1, 0), (0, 1, 0)), 3)
    parts2 = [row_copies(hood2, flat_faces, by, gs, gr) for by in range(SBY)]

    def kick_drift(c, p, tile, force):
        v = vbuf[c] + (2.0 * inner_step) * force
        vbuf[c] = v
        hood2[p] = tile + inner_step * v

    for d in ORDER[:ORDER_Y]:
        take1(d)

    def first_row(g, _):
        by = jnp.where(g == 0, 1, jnp.where(g == 1, 0, jnp.where(g == 2, SBY - 1, 2)))
        pair_row(hood1, by, kick_drift)

        @pl.when(g == 0)
        def _():
            for d in ORDER[ORDER_Y:]:
                take1(d)

        @pl.when(g == 1)
        def _():
            copies2[(0, -1, 0)].start()

        @pl.when(g == 2)
        def _():
            copies2[(0, 1, 0)].start()

        for copy in row_copies(hood2, flat_faces, by, gs, gr).values():
            copy.start()
        return 0

    lax.fori_loop(0, SBY, first_row, 0)
    copies3 = halo(hood3, 3, [d for d in AROUND if d[1] != 0], 3)
    flat_around = [d for d in AROUND if d[1] == 0]
    parts3 = [row_copies(hood3, flat_around, by, rs, rr) for by in range(SBY)]
    bond_inside(hood2, inner_step)
    for by in (1, SBY - 1, 0, 2):
        for d in flat_faces:
            parts2[by][d].wait_recv()
            bond_face(hood2, inner_step, d, (by, 1))
        if by in (0, SBY - 1):
            d = (0, 1, 0) if by == 0 else (0, -1, 0)
            copies2[d].wait_recv()
            bond_face(hood2, inner_step, d)
        drift(hood2, hood3, by)
        if by in (0, SBY - 1):
            launch({d: copies3[d] for d in copies3 if d[1] == (-1 if by == 0 else 1)})
        launch(parts3[by])
    cell_ids = lax.broadcasted_iota(jnp.int32, (8, BLK), 0) * BLK + lax.broadcasted_iota(
        jnp.int32, (8, BLK), 1
    )
    corner = rows4(
        (me[0] * SBX).astype(F32), (me[1] * SBY).astype(F32), (me[2] * SBZ).astype(F32), 0.0
    )

    def gather_moments(b, totals):
        px, py, pz = place(b)
        tile = hood3[px, py, pz]
        for d in range(3):
            oo[d, b] = tile[d : d + 1]
        sums = jnp.sum(
            qbuf[b] * jnp.where(xyz, tile + corner, 1.0), axis=1, keepdims=True
        )
        here = cell_ids == cell[b]
        return tuple(
            total + jnp.where(here, sums[d : d + 1], 0.0) for d, total in enumerate(totals)
        )

    zero = jnp.zeros((8, BLK), F32)
    moments = lax.fori_loop(0, NB, gather_moments, (zero, zero, zero, zero), unroll=16)
    for d in range(4):
        part0[d] = moments[d]

    stages = ((2, 4, part0, got0, 0), (0, 4, part1, got1, 3), (1, 8, part2, got2, 6))

    def spread(stage):
        axis, n, mine, got, base = stages[stage]
        return [
            pltpu.make_async_remote_copy(
                src_ref=mine,
                dst_ref=got.at[o - 1],
                send_sem=ms.at[base + o - 1],
                recv_sem=mr.at[base + o - 1],
                device_id=device(tuple(o if a == axis else 0 for a in range(3))),
                device_id_type=MESH,
            )
            for o in range(1, n)
        ]

    spreads = [spread(stage) for stage in range(3)]

    def send_moments(stage):
        for copy in spreads[stage]:
            copy.start()

    def collect(stage):
        axis, n, mine, got, base = stages[stage]
        for copy in spreads[stage]:
            copy.wait_recv()
        total = mine[...]
        for o in range(1, n):
            total = total + got[o - 1]
        return total

    send_moments(0)
    bond_inside(hood3, half_step)
    prepare_own(hood3)
    drained([copies1, copies2] + parts2)

    def take3(copies, d, rows=(0, SBY)):
        copies[d].wait_recv()
        prepare_ghosts(hood3, d, rows)
        if d in FACES:
            bond_face(hood3, half_step, d, rows)

    def kick(c, p, tile, force):
        vbuf[c] = vbuf[c] + inner_step * force

    for by in (1, SBY - 1, 0):
        for d in flat_around:
            take3(parts3[by], d, (by, 1))
    part1[...] = collect(0)
    send_moments(1)
    for d in ORDER[ORDER_Y:]:
        if d[1] > 0:
            take3(copies3, d)

    def second_row(by, _):
        pair_row(hood3, by, kick)

        @pl.when(by == 0)
        def _():
            for d in flat_around:
                take3(parts3[2], d, (2, 1))
            for d in ORDER[ORDER_Y:]:
                if d[1] < 0:
                    take3(copies3, d)

        @pl.when(by == 0)
        def _():
            part2[...] = collect(1)
            send_moments(2)

        return 0

    lax.fori_loop(0, SBY, second_row, 0)
    drained([copies3] + parts3 + spreads[:2])
    totals = collect(2)

    charge_sum = totals[3]
    places = [centre[d] for d in range(3)]
    dipole = [totals[d] - charge_sum * places[d] for d in range(3)]

    def finish(b, _):
        target = cell[b]
        away = [
            frac_s[d, target] * (1.0 * SIZES[d] * (SBX, SBY, SBZ)[d]) - places[d]
            for d in range(3)
        ]
        inverse = lax.rsqrt(
            away[0] * away[0] + away[1] * away[1] + away[2] * away[2] + soften * soften
        )
        cube = inverse * inverse * inverse
        fifth = cube * inverse * inverse
        along = dipole[0] * away[0] + dipole[1] * away[1] + dipole[2] * away[2]
        gain = charge_sum * cube + 3.0 * along * fifth
        field = [
            jnp.sum(gain * away[d] - dipole[d] * cube, axis=(0, 1), keepdims=True)
            for d in range(3)
        ]
        size = (outer_half * coulomb) * qbuf[b]
        v = vbuf[b]
        for d in range(3):
            oo[3 + d, b] = v[d : d + 1] + size * field[d]
        return 0

    lax.fori_loop(0, NB, finish, 0, unroll=32)

    drained(spreads[2:])


def per_device(
    positions,
    velocities,
    strength,
    charge,
    bond_stiffness,
    bond_partner,
    pair_blocks,
    tile_count,
    block_cell,
    cell_frac,
    bond_force,
    pair_force,
    far_force,
):
    lines = lambda value, n: value.reshape(n, NB, 1, BLK)
    vmem = pl.BlockSpec(memory_space=pltpu.VMEM)
    anywhere = pl.BlockSpec(memory_space=pl.ANY)
    hood = pltpu.VMEM((EX, EY, EZ, 4, BLK), F32)
    line3 = pltpu.VMEM((3, NB, 1, BLK), F32)
    line2 = pltpu.VMEM((2, NB, 1, BLK), F32)
    line1 = pltpu.VMEM((NB, 1, BLK), F32)
    sums = pltpu.VMEM((4, 8, BLK), F32)
    out = jax.ShapeDtypeStruct((3, NB, 1, BLK), F32)
    xv = pl.pallas_call(
        kernel,
        out_shape=jax.ShapeDtypeStruct((6, NB, 1, BLK), F32),
        in_specs=[anywhere] * 13,
        out_specs=vmem,
        scratch_shapes=[
            line3,
            line3,
            line1,
            line1,
            line2,
            pltpu.VMEM((2, NB, 1, BLK), jnp.int32),
            line3,
            line3,
            line3,
            pltpu.VMEM((3, CELLS), F32),
            pltpu.SMEM((3, CELLS), F32),
            pltpu.SMEM((8, NB), jnp.int32),
            pltpu.SMEM((NB,), jnp.int32),
            pltpu.SMEM((1,), jnp.int32),
            hood,
            hood,
            hood,
            hood,
            pltpu.VMEM((NB, 4, BLK), F32),
            line1,
            pltpu.VMEM((NB, 8, BLK), jnp.int32),
            pltpu.VMEM((NB, 8, BLK), jnp.int32),
            pltpu.VMEM((NB, 8, BLK), F32),
            pltpu.VMEM((NE, 32, BLK), BF16),
            pltpu.VMEM((NE, 16, BLK), BF16),
            pltpu.VMEM((NB, BLK, 32), BF16),
            pltpu.VMEM((3, 8, BLK), F32),
            sums,
            sums,
            sums,
            pltpu.VMEM((3, 4, 8, BLK), F32),
            pltpu.VMEM((3, 4, 8, BLK), F32),
            pltpu.VMEM((7, 4, 8, BLK), F32),
            pltpu.SemaphoreType.DMA((14,)),
            pltpu.SemaphoreType.DMA((4, 26)),
            pltpu.SemaphoreType.DMA((4, 26)),
            pltpu.SemaphoreType.DMA((4, 4)),
            pltpu.SemaphoreType.DMA((4, 4)),
            pltpu.SemaphoreType.DMA((4, 8)),
            pltpu.SemaphoreType.DMA((4, 8)),
            pltpu.SemaphoreType.DMA((13,)),
            pltpu.SemaphoreType.DMA((13,)),
        ],
        compiler_params=pltpu.CompilerParams(
            collective_id=0, has_side_effects=True, vmem_limit_bytes=60 * 1024 * 1024
        ),
        name="outer_step",
    )(
        lines(positions, 3),
        lines(velocities, 3),
        strength.reshape(NB, 1, BLK),
        charge.reshape(NB, 1, BLK),
        lines(bond_stiffness, 2),
        lines(bond_partner, 2),
        lines(bond_force, 3),
        lines(pair_force, 3),
        lines(far_force, 3),
        cell_frac,
        pair_blocks.reshape(NB, 8).T,
        block_cell.reshape(NB),
        tile_count.reshape(1),
    )
    return xv[:3].reshape(positions.shape), xv[3:].reshape(velocities.shape)


def solution(mesh):
    vector = P(None, "gx", "gy", "gz", None)
    scalar = P("gx", "gy", "gz", None)
    in_specs = (
        vector,
        vector,
        scalar,
        scalar,
        vector,
        vector,
        P("gx", "gy", "gz", None, None),
        P("gx", "gy", "gz"),
        scalar,
        P(),
        vector,
        vector,
        vector,
    )
    return jax.shard_map(
        per_device, mesh=mesh, in_specs=in_specs, out_specs=(vector, vector), check_vma=False
    )
```
